32 devices in a mesh: cache: 4 (over x, core), expert: 8 (over z, y).
Axes of the slice: x: 2, y: 2, z: 4, core: 2. Of those that a mesh axis runs over, the one named last changes fastest.
Arguments:
- queries: bfloat16 [2, 32, 2048], P(None, 'expert'), may hold values from -16 to 16
- k_cache: bfloat16 [32, 4096, 256], P('expert', 'cache'), may hold values from -6 to 6
- v_cache: bfloat16 [32, 4096, 256], P('expert', 'cache'), may hold values from -6 to 6
- lengths: int32 [32], P('expert'), may hold values from 1 to 4094
- w_out: bfloat16 [2048, 2880], P('cache'), may hold values from -0.125 to 0.125
- norm_gain: float32 [2880], replicated, may hold values from 0.25 to 1.75
- w_gate: bfloat16 [8, 2880, 1440], P('cache', 'expert'), may hold values from -0.109375 to 0.109375
- w_up: bfloat16 [8, 2880, 1440], P('cache', 'expert'), may hold values from -0.109375 to 0.109375
- w_down: bfloat16 [8, 1440, 2880], P('cache', None, 'expert'), may hold values from -0.15625 to 0.15625
- expert_ids: int32 [2, 32, 4], P(None, 'expert'), may hold values from 0 to 7, all different within a row; in each aligned block of 4 rows (0 to 3, 4 to 7, ..., all dimensions but the last counted through in order) at most 2 rows name the same one
- gate_weights: float32 [2, 32, 4], P(None, 'expert'), may hold values from 0.1 to 1
Outputs:
- mixed: bfloat16 [2, 32, 2880], P(None, 'expert')
- gate_owner: bfloat16 [8, 2880, 1440], P('expert', None, 'cache')
- up_owner: bfloat16 [8, 2880, 1440], P('expert', None, 'cache')
- down_owner: bfloat16 [8, 1440, 2880], P('expert', 'cache')
The draws below stay inside these ranges and needn't reach their ends.
Inputs may be any that keep to these rules, and one draw needn't show every extreme that they name: `expert_ids`: in each step the 4 rows of one index of expert name one expert at most 2 times; a row names 4 different experts.
All inputs are finite; a program needn't handle non-finite values.
Results may differ from the reference program's by a relative error of at most 0.015.
Values may be sent and summed in bfloat16 or wider, within the bound.
A program may use at most 64 MiB of HBM per device.

```python
import math
import jax
import jax.numpy as jnp
import numpy as np
from jax import lax

D = 2880
FF = 1440
QH = 32
KVH = 4
HD = 64
TOP = 4
STEPS = 2
ROWS_DEV = 4
EXPERTS = 8
CAP = 2
ROWS = 32
LENGTH = 4096


def draw_queries(key, part):
    result = 2.5 * jax.random.truncated_normal(jax.random.fold_in(key, 1), -6.0, 6.0, (STEPS, ROWS, QH * HD), jnp.float32)
    return result.astype(jnp.bfloat16)


def draw_k_cache(key, part):
    result = jax.random.truncated_normal(jax.random.fold_in(key, 2), -6.0, 6.0, (ROWS, LENGTH, KVH * HD), jnp.float32)
    return result.astype(jnp.bfloat16)


def place_ends(values, rng, low, top_value):
    longest = values.shape.index(max(values.shape))
    spots = []
    for shift in (0, 1):
        where = [jax.random.randint(jax.random.fold_in(rng, axis), (), 0, length) for axis, length in enumerate(values.shape)]
        where[longest] = (where[longest] + shift) % values.shape[longest]
        spots.append(tuple(where))
    return values.at[spots[0]].set(low).at[spots[1]].set(top_value)


def steps_of(own_key, dims, cuts, smallest, top_value):
    gain, own = 1.0, jax.random.fold_in(own_key, 6)
    for dim, shards_of in cuts:
        draws = jnp.exp(jax.random.uniform(jax.random.fold_in(own, dim), (shards_of,), jnp.float32, smallest / len(cuts), top_value / len(cuts)))
        gain = gain * jnp.repeat(draws, dims[dim] // shards_of).reshape([-1 if axis == dim else 1 for axis in range(len(dims))])
    return gain


def deal_out(own_key, own, number, rows, count, top, bound, skew):
    sequence = jax.random.permutation(own_key, count)
    heavy_load, common = shares(count, rows * top, bound, skew, True), shares(count, rows * top, bound, skew, False)
    places = jnp.arange(count)

    def named(tallies, rotation):
        used = int((tallies > 0).sum())
        fixed = max(1, used // 4)
        moved = fixed + (places - fixed + rotation * (used - fixed)) % max(1, count - fixed)
        return jnp.zeros((count,), jnp.int32).at[sequence[jnp.where(places < fixed, places, moved)]].set(jnp.asarray(tallies, jnp.int32))

    tallies = jnp.where(number % 4 == 0, named(heavy_load, number // 4), named(common, number - number // 4 - 1))
    mixed = jax.random.permutation(jax.random.fold_in(own, 3), count)
    donor, taker = mixed[0:count // 2 * 2:2], mixed[1:count // 2 * 2:2]
    margin = jnp.minimum(tallies[donor] - 1, bound - tallies[taker]) // 2
    margin = jnp.where((donor == sequence[0]) | (taker == sequence[0]) | (tallies[taker] == 0), 0, jnp.maximum(margin, 0))
    moved = jax.random.randint(jax.random.fold_in(own, 4), (count // 2,), 0, 1 << 20) % (margin + 1)
    tallies = tallies.at[donor].add(-moved).at[taker].add(moved)
    labels = jnp.searchsorted(jnp.cumsum(tallies), jnp.arange(rows * top), side="right").astype(jnp.int32)
    listing = labels.reshape(top, rows).T
    listing = listing[jax.random.permutation(jax.random.fold_in(own, 1), rows)]
    rotation = jax.random.randint(jax.random.fold_in(own, 2), (rows, 1), 0, top)
    return jnp.take_along_axis(listing, (jnp.arange(top)[None, :] + rotation) % top, axis=1)


def shares(count, total, most, skew, full):
    weights = [(1 << 20) // math.isqrt(grade ** skew) + 1 for grade in range(1, count + 1)]
    largest = most if full else min(most, max(-(-total // count), total * weights[0] // sum(weights)))
    least = 1 if total - largest >= count - 1 else 0
    holding, spare = [largest] + [least] * (count - 1), total - largest - least * (count - 1)
    while spare > 0:
        free = [i for i in range(1, count) if holding[i] < largest] or [i for i in range(1, count) if holding[i] < most]
        whole, left = sum([weights[i] for i in free]), spare
        for i in free:
            addition = min(most - holding[i], max(1, left * weights[i] // whole), spare)
            holding[i] = holding[i] + addition
            spare = spare - addition
    return np.array(holding)


def gaussian(key, dims, deviation, reach, shards=(), kind=jnp.bfloat16):
    values = deviation * jax.random.normal(key, dims, jnp.float32)
    if shards:
        values = values * steps_of(key, dims, shards, -0.22, 0.18)
    return jnp.clip(values, -reach, reach).astype(kind)


def setup_inputs(seed: int = 0) -> dict:
    splits = jax.random.split(jax.random.key(seed), 12)
    queries = draw_queries(jax.random.fold_in(splits[11], 71), 0)
    k_cache = draw_k_cache(jax.random.fold_in(splits[11], 71), 0)
    v_cache = gaussian(splits[2], (ROWS, LENGTH, KVH * HD), 1.0, 6.0, ((0, 8), (1, 4)))
    lengths = place_ends(jax.random.randint(splits[3], (ROWS,), 1, LENGTH - 1), jax.random.fold_in(splits[3], 1), 1, (LENGTH - 1) - 1).astype(jnp.int32)
    w_out = gaussian(splits[4], (QH * HD, D), (QH * HD) ** -0.5, 0.125, ((0, 4),))
    norm_gain = jnp.clip(1.0 + 0.15 * jax.random.normal(splits[5], (D,), jnp.float32), 0.25, 1.75)
    w_gate = gaussian(splits[6], (EXPERTS, D, FF), D ** -0.5, 0.109375, ((0, 4), (1, 8)))
    w_up = gaussian(splits[7], (EXPERTS, D, FF), D ** -0.5, 0.109375, ((0, 4), (1, 8)))
    w_down = gaussian(splits[8], (EXPERTS, FF, D), FF ** -0.5, 0.15625, ((0, 4), (2, 8)))
    expert_ids_keys = jax.random.split(jax.random.fold_in(splits[9], 1), STEPS * ROWS // ROWS_DEV)
    expert_ids_turns = jax.random.permutation(jax.random.fold_in(splits[9], 3), STEPS * ROWS // ROWS_DEV)
    expert_ids = jax.vmap(lambda own, number: deal_out(jax.random.fold_in(splits[9], 2), own, number, ROWS_DEV, EXPERTS, TOP, CAP, 2))(expert_ids_keys, expert_ids_turns).reshape((STEPS, ROWS, TOP))
    gate_weights = jnp.clip(0.1 + 0.9 * jax.random.uniform(splits[10], (STEPS, ROWS, TOP), jnp.float32) ** steps_of(splits[10], (STEPS, ROWS, TOP), ((1, 8),), -0.2, 0.2), 0.1, 1.0)
    return {"queries": queries, "k_cache": k_cache, "v_cache": v_cache, "lengths": lengths, "w_out": w_out, "norm_gain": norm_gain, "w_gate": w_gate, "w_up": w_up, "w_down": w_down, "expert_ids": expert_ids, "gate_weights": gate_weights}


def attend_row(query_row, key_row, value_row, length_row):
    group_size = QH // KVH
    query_heads = query_row.astype(jnp.float32).reshape(STEPS, KVH, group_size, HD)
    key_heads = key_row.astype(jnp.float32).reshape(LENGTH, KVH, HD)
    value_heads = value_row.astype(jnp.float32).reshape(LENGTH, KVH, HD)
    scores = jnp.einsum('shgd,phd->shgp', query_heads, key_heads) / math.sqrt(HD)
    limit = length_row + jnp.arange(STEPS, dtype=jnp.int32) + 1
    visible = jnp.arange(LENGTH, dtype=jnp.int32)[None, :] < limit[:, None]
    visible = visible[:, None, None, :]
    highest = lax.optimization_barrier(jnp.max(jnp.where(visible, scores, -1e+30), axis=-1, keepdims=True))
    weights = jnp.where(visible, jnp.exp(scores - highest), 0.0)
    mass = lax.optimization_barrier(jnp.sum(weights, axis=-1))
    rounded = lax.optimization_barrier(weights.astype(jnp.bfloat16)).astype(jnp.float32)
    accum = jnp.einsum('shgp,phd->shgd', rounded, value_heads)
    return (accum / mass[..., None]).reshape(STEPS, QH * HD).astype(jnp.bfloat16)

def reference(queries, k_cache, v_cache, lengths, w_out, norm_gain, w_gate, w_up, w_down, expert_ids, gate_weights):
    outputs = lax.map(lambda inputs: attend_row(*inputs), (jnp.swapaxes(queries, 0, 1), k_cache, v_cache, lengths))
    heads_out = jnp.swapaxes(outputs, 0, 1).reshape(STEPS * ROWS, QH * HD)
    attention = jnp.dot(heads_out, w_out, preferred_element_type=jnp.float32)
    scale = lax.rsqrt(lax.optimization_barrier(jnp.mean(attention * attention, axis=-1, keepdims=True)) + 1e-05)
    normed = (attention * scale * norm_gain).astype(jnp.bfloat16)
    picked = (expert_ids[..., None] == jnp.arange(EXPERTS, dtype=jnp.int32)).astype(jnp.float32)
    coefficient = lax.optimization_barrier(jnp.sum(picked * gate_weights[..., None], axis=2)).reshape(STEPS * ROWS, EXPERTS)

    def one_expert(running, inputs):
        gate_matrix, up_matrix, down_matrix, column = inputs
        gate_value = jnp.dot(normed, gate_matrix, preferred_element_type=jnp.float32)
        up_value = jnp.dot(normed, up_matrix, preferred_element_type=jnp.float32)
        hidden = (jax.nn.silu(gate_value) * up_value).astype(jnp.bfloat16)
        expert_out = jnp.dot(hidden, down_matrix, preferred_element_type=jnp.float32).astype(jnp.bfloat16)
        expert_out = lax.optimization_barrier(expert_out).astype(jnp.float32)
        return (running + column[:, None] * expert_out, None)
    start = jnp.zeros((STEPS * ROWS, D), jnp.float32)
    combined, _ = lax.scan(one_expert, start, (w_gate, w_up, w_down, coefficient.T))
    mixed = (attention + combined).astype(jnp.bfloat16).reshape(STEPS, ROWS, D)
    return (mixed, w_gate, w_up, w_down)
```

```python
import functools
import math

import jax
import jax.numpy as jnp
from jax import lax
from jax.experimental import pallas as pl
from jax.experimental.pallas import tpu as pltpu
from jax.sharding import PartitionSpec as P

D = 2880
QH = 32
KVH = 4
HD = 64
TOP = 4
NEAR = 2

MESH = pl.DeviceIdType.MESH
F32 = jnp.float32
BF16 = jnp.bfloat16


def dot_nt(a, b):
    return lax.dot_general(a, b, (((1,), (1,)), ((), ())), preferred_element_type=F32)


def dot_nn(a, b):
    return jnp.dot(a, b, preferred_element_type=F32)


def iota(shape, axis):
    return lax.broadcasted_iota(jnp.int32, shape, axis)


def whole_kernel(
    C, E, I, S, R, cap,
    lengths, ids, gates, q_ref, gain_ref, k_hbm, v_hbm, wo_hbm, wg_hbm, wu_hbm, wd_hbm,
    g_own, u_own, d_own, mixed_ref,
    g_in, u_in, d_in, g_stage, u_stage, relay_g, relay_u, relay_d, fin_g, fin_u, fin_d,
    k_in, v_in, wo_in, q_f32, part_out, part_in, proj, normed, out_slots, in_slots, slots_bf, slots_all,
    rows_x, hid_out, hid_in, back_out, back_in, comb,
    load_sem, sx, r1, sd, sr, rf, loc, s_part, r_part, s_proj, r_proj, s_disp, r_disp, s_slot, r_slot,
    s_hid, r_hid, s_back, r_back, s_comb, r_comb,
):
    c = lax.axis_index("cache")
    e = lax.axis_index("expert")
    x = c // NEAR
    k = lax.rem(c, NEAR)
    O = C - NEAR
    width = g_own.shape[0]
    rows = fin_g.shape[2]
    group = QH // KVH
    per_row = group * S
    heads_rows = KVH * per_row
    items = S * cap
    total = S * R
    chunk = out_slots.shape[1] * 2
    half = chunk // 2
    d_model = E * rows

    loads = []
    for i in range(I):
        loads.append(pltpu.make_async_copy(wg_hbm.at[i], g_in.at[i], load_sem.at[0, i]))
    loads.append(pltpu.make_async_copy(k_hbm, k_in, load_sem.at[3, 0]))
    loads.append(pltpu.make_async_copy(v_hbm, v_in, load_sem.at[3, 1]))
    for i in range(I):
        loads.append(pltpu.make_async_copy(wu_hbm.at[i], u_in.at[i], load_sem.at[1, i]))
    loads.append(pltpu.make_async_copy(wd_hbm, d_in, load_sem.at[2, 0]))
    loads.append(pltpu.make_async_copy(wo_hbm, wo_in, load_sem.at[2, 1]))
    for load in loads:
        load.start()
    load_g, load_k, load_v = loads[:I], loads[I], loads[I + 1]
    load_u, load_d, load_wo = loads[I + 2 : 2 * I + 2], loads[2 * I + 2], loads[2 * I + 3]

    barrier = pltpu.get_barrier_semaphore()
    me = c * E + e
    for n in range(1, C * E):
        other = lax.rem(me + n, C * E)
        pl.semaphore_signal(barrier, inc=1, device_id=(other // E, lax.rem(other, E)), device_id_type=MESH)
    pl.semaphore_wait(barrier, C * E - 1)

    relays = (relay_g, relay_u, relay_d)
    finals = (fin_g, fin_u, fin_d)

    def remote(src, dst, send, recv, tc, te):
        return pltpu.make_async_remote_copy(
            src_ref=src, dst_ref=dst, send_sem=send, recv_sem=recv, device_id=(tc, te), device_id_type=MESH
        )

    def block(w, i, target):
        return (g_stage, u_stage, d_in)[w].at[i, target]

    def far(o):
        return lax.rem(x * NEAR + NEAR + o, C)

    def direct(w, i, kd, action):
        target = x * NEAR + kd
        owner = c * I + i
        own = (owner == e) & (k == kd)

        @pl.when(own)
        def _():
            if action == "start":
                pltpu.make_async_copy(block(w, i, target), finals[w].at[e], loc.at[w]).start()

        @pl.when(jnp.logical_not(own))
        def _():
            copy = remote(block(w, i, target), finals[w].at[e], sd.at[w, i, kd], rf.at[w, e], target, owner)
            copy.start() if action == "start" else copy.wait_send()

    def hop(w, i, o, action):
        target = far(o)
        owner = c * I + i
        place = lax.rem(c - (target // NEAR) * NEAR - NEAR + 2 * C, C)

        @pl.when(owner == e)
        def _():
            copy = remote(block(w, i, target), finals[w].at[e], sx.at[w, i, o], rf.at[w, e], target, e)
            copy.start() if action == "start" else copy.wait_send()

        @pl.when(owner != e)
        def _():
            copy = remote(block(w, i, target), relays[w].at[place, i], sx.at[w, i, o], r1.at[w, place, i], target, e)
            copy.start() if action == "start" else copy.wait_send()

    def pass_on(w, o, i, action):
        owner = far(o) * I + i

        @pl.when(owner != e)
        def _():
            part = relays[w].at[o, i]
            copy = remote(part, finals[w].at[e], sr.at[w, o, i], rf.at[w, e], c, owner)
            if action == "start":
                remote(part, part, sr.at[w, o, i], r1.at[w, o, i], c, owner).wait_recv()
                copy.start()
            else:
                copy.wait_send()

    def arrived(w, s):
        own = (c == e // I) & (e == s)

        @pl.when(own)
        def _():
            pltpu.make_async_copy(finals[w].at[s], finals[w].at[s], loc.at[w]).wait()

        @pl.when(jnp.logical_not(own))
        def _():
            remote(finals[w].at[s], finals[w].at[s], sd.at[w, 0, 0], rf.at[w, s], c, s).wait_recv()

    def stage(w, i):
        source, target = (g_in, u_in)[w], (g_stage, u_stage)[w]
        for t in range(C):
            target[i, t] = source[i, :, t * width : (t + 1) * width].T

    def put_together(w):
        own = (g_own, u_own, d_own)[w]
        for s in range(E):
            arrived(w, s)
            own[:, s * rows : (s + 1) * rows] = finals[w][s]

    for i in range(I):
        load_g[i].wait()
        stage(0, i)
        for o in range(O):
            hop(0, i, o, "start")
        for kd in range(NEAR):
            direct(0, i, kd, "start")

    for s in range(S):
        q_f32[s * R : (s + 1) * R, :] = q_ref[s].astype(F32)
    lane_q = iota((heads_rows, QH * HD), 1)
    row_q = iota((heads_rows, QH * HD), 0)
    head_of_row = (row_q // per_row) * group + lax.rem(row_q, per_row) // S
    mine = (lane_q // HD) == head_of_row
    step_q = lax.rem(row_q, S)
    fold_l = iota((QH * HD, KVH * HD), 0)
    fold_m = iota((QH * HD, KVH * HD), 1)
    fold = ((lax.rem(fold_l, HD) == lax.rem(fold_m, HD)) & (fold_l // (group * HD) == fold_m // HD)).astype(F32).astype(BF16)
    load_k.wait()
    load_v.wait()
    positions = k_in.shape[1]
    place_of = c * positions + iota((heads_rows, positions), 1)
    step_p = lax.rem(iota((heads_rows, positions), 0), S)
    lane_t = iota((per_row, 128), 1)
    for r in range(R):
        rows_q = q_f32[r : r + 1, :]
        spread = jnp.broadcast_to(rows_q, (heads_rows, QH * HD))
        for s in range(1, S):
            spread = jnp.where(step_q == s, jnp.broadcast_to(q_f32[s * R + r : s * R + r + 1, :], spread.shape), spread)
        spread = jnp.where(mine, spread, 0.0).astype(BF16)
        spread = dot_nn(spread, fold).astype(BF16)
        score = dot_nt(spread, k_in[r]) * (1.0 / math.sqrt(HD))
        visible = place_of < lengths[r] + step_p + 1
        highest = jnp.max(jnp.where(visible, score, -1e30), axis=1, keepdims=True)
        weight = jnp.where(visible, jnp.exp(score - highest), 0.0)
        mass = jnp.sum(weight, axis=1, keepdims=True)
        accum = dot_nn(weight.astype(BF16), v_in[r])
        for h in range(KVH):
            span = slice(h * per_row, (h + 1) * per_row)
            base = (h * HD // 128) * 128
            piece = accum[span, base : base + 128]
            if h * HD % 128:
                piece = pltpu.roll(piece, 128 - HD, 1)
            piece = jnp.where(lane_t < HD, piece, jnp.where(lane_t < HD + 32, highest[span], mass[span]))
            part_out[h, r * per_row : (r + 1) * per_row, :] = piece

    def part(n, action):
        target = lax.rem(c + n, C)
        if action == "recv":
            remote(part_in.at[target], part_in.at[target], s_part.at[target], r_part.at[target], target, e).wait_recv()
            return
        copy = remote(part_out.at[target], part_in.at[c], s_part.at[target], r_part.at[c], target, e)
        copy.start() if action == "start" else copy.wait_send()

    for n in range(1, C):
        part(n, "start")
    part_in[c] = part_out[c]

    for i in range(I):
        load_u[i].wait()
        stage(1, i)
        for o in range(O):
            hop(1, i, o, "start")
        for o in range(O):
            pass_on(0, o, i, "start")
        for kd in range(NEAR):
            direct(1, i, kd, "start")

    def table(shape, row_axis):
        row = iota(shape, row_axis)
        slot = iota(shape, 1 - row_axis)
        expert = slot // (2 * items)
        inside = lax.rem(slot, items)
        chosen = jnp.zeros(shape, F32)
        weight = jnp.zeros(shape, F32)
        for s in range(S):
            for r in range(R):
                for t in range(TOP):
                    hit = (row == s * R + r) & (expert == ids[s, r, t])
                    chosen = jnp.where(hit, 1.0, chosen)
                    weight = jnp.where(hit, gates[s, r, t], weight)
        rank = jnp.zeros(shape, F32)
        place = lax.rem(row, R)
        for n in range(1, R):
            rank = rank + jnp.where(place >= n, pltpu.roll(chosen, n, row_axis), 0.0)
        fit = (row < total) & (inside // cap == row // R) & (rank == lax.rem(inside, cap).astype(F32))
        chosen = jnp.where(fit, chosen, 0.0)
        return chosen, weight * chosen

    send_table, _ = table((E * 2 * items, 128), 1)
    _, gate_table = table((total, 128), 0)

    for n in range(1, C):
        part(n, "recv")
    tall = R * per_row
    top = part_in[0][:, HD : HD + 1]
    for s in range(1, C):
        top = jnp.maximum(top, part_in[s][:, HD : HD + 1])
    number = jnp.zeros((tall, 128), F32)
    mass = jnp.zeros((tall, 1), F32)
    for s in range(C):
        one = part_in[s]
        factor = jnp.exp(one[:, HD : HD + 1] - top)
        number = number + one * factor
        mass = mass + one[:, HD + 32 : HD + 33] * factor
    number = number / mass
    lane_h = iota((tall, 128), 1)
    number = jnp.where(lane_h < HD, number, pltpu.roll(number, HD, 1))
    number = jnp.concatenate([number] * (group * HD // 128), axis=1)
    lane_w = iota(number.shape, 1)
    row_w = iota(number.shape, 0)
    number = jnp.where(lane_w // HD == lax.rem(row_w, per_row) // S, number, 0.0).astype(BF16)
    row_s = iota((total, tall), 0)
    col_s = iota((total, tall), 1)
    gather = ((col_s // per_row == lax.rem(row_s, R)) & (lax.rem(col_s, S) == row_s // R)).astype(F32).astype(BF16)
    heads_out = dot_nn(gather, number).astype(BF16)
    load_wo.wait()
    proj[c] = dot_nt(heads_out, wo_in[...])

    def gather_cache(buffer, send, recv, n, action):
        target = lax.rem(c + n, C)
        if action == "recv":
            remote(buffer.at[target], buffer.at[target], send.at[target], recv.at[target], target, e).wait_recv()
            return
        copy = remote(buffer.at[c], buffer.at[c], send.at[target], recv.at[c], target, e)
        copy.start() if action == "start" else copy.wait_send()

    for n in range(1, C):
        gather_cache(proj, s_proj, r_proj, n, "start")

    load_d.wait()
    for i in range(I):
        for o in range(O):
            hop(2, i, o, "start")
    for i in range(I):
        for o in range(O):
            pass_on(1, o, i, "start")
    for n in range(1, C):
        gather_cache(proj, s_proj, r_proj, n, "recv")
    attention = proj[0]
    for s in range(1, C):
        attention = attention + proj[s]
    scale = lax.rsqrt(jnp.sum(attention * attention, axis=1, keepdims=True) * (1.0 / d_model) + 1e-05)
    normed[:, d_model:] = jnp.zeros((total, C * chunk - d_model), F32)
    normed[:, :d_model] = (attention * scale * gain_ref[...]).astype(BF16).astype(F32)
    own_chunk = normed[:, pl.ds(pl.multiple_of(c * chunk, 128), chunk)]
    placed = dot_nn(send_table[:, :total], own_chunk)
    upper = lax.rem(iota((E * 2 * items, half), 0), 2 * items) < items
    out_slots[...] = jnp.where(upper, placed[:, :half], placed[:, half:])
    step8 = 2 * items

    def at_expert(buffer, index):
        return buffer.at[pl.ds(pl.multiple_of(index * step8, step8), step8)]

    def spread_expert(out, back, send, recv, n, action):
        target = lax.rem(e + n, E)
        if action == "recv":
            spot = at_expert(back, target)
            remote(spot, spot, send.at[target], recv.at[target], c, target).wait_recv()
            return
        copy = remote(at_expert(out, target), at_expert(back, e), send.at[target], recv.at[e], c, target)
        copy.start() if action == "start" else copy.wait_send()

    for n in range(1, E):
        spread_expert(out_slots, in_slots, s_disp, r_disp, n, "start")
    in_slots[pl.ds(pl.multiple_of(e * step8, step8), step8), :] = out_slots[pl.ds(pl.multiple_of(e * step8, step8), step8), :]

    direct(2, 0, 0, "start")
    direct(2, 0, 1, "start")
    for i in range(I):
        for o in range(O):
            pass_on(2, o, i, "start")
    for n in range(1, E):
        spread_expert(out_slots, in_slots, s_disp, r_disp, n, "recv")
    slots_all[c] = in_slots[...].astype(BF16)
    for n in range(1, C):
        gather_cache(slots_all, s_slot, r_slot, n, "start")
    for n in range(1, C):
        gather_cache(slots_all, s_slot, r_slot, n, "recv")
    count = E * items
    row_t = iota((count, 2 * count), 0)
    col_t = iota((count, 2 * count), 1)
    base = (row_t // items) * step8 + lax.rem(row_t, items)
    take_low = (col_t == base).astype(F32).astype(BF16)
    take_high = (col_t == base + items).astype(F32).astype(BF16)
    for s in range(C):
        rows_x[:, s * chunk : s * chunk + half] = dot_nn(take_low, slots_all[s]).astype(BF16)
        rows_x[:, s * chunk + half : (s + 1) * chunk] = dot_nn(take_high, slots_all[s]).astype(BF16)

    put_together(0)
    gate_value = dot_nt(rows_x[:, :d_model], g_own[...])
    put_together(1)
    up_value = dot_nt(rows_x[:, :d_model], u_own[...])
    hid_out[...] = (gate_value * jax.nn.sigmoid(gate_value) * up_value).astype(BF16)

    column = e // I
    inner = lax.rem(e, I)

    def hidden(n, action):
        target = lax.rem(e + n, E)
        own = (column == c) & (target == e)

        @pl.when(jnp.logical_not(own))
        def _():
            copy = remote(hid_out, hid_in.at[inner, c], s_hid.at[target], r_hid.at[inner, c], column, target)
            copy.start() if action == "start" else copy.wait_send()

        if n == 0 and action == "start":

            @pl.when(own)
            def _():
                hid_in[inner, c] = hid_out[...]

    for n in range(E):
        hidden(n, "start")
    for i in range(1, I):
        for kd in range(NEAR):
            direct(2, i, kd, "start")
    down = []
    for i in range(I):
        value = jnp.zeros((count, rows), F32)
        for s in range(C):
            @pl.when(jnp.logical_not((s == c) & (e == c * I + i)))
            def _():
                remote(hid_in.at[i, s], hid_in.at[i, s], s_hid.at[0], r_hid.at[i, s], s, e).wait_recv()
            value = value + dot_nn(hid_in[i, s], d_in[i, s])
        down.append(value.astype(BF16))
    row_b = iota((I * count, count), 0)
    col_b = iota((I * count, count), 1)
    back = jnp.zeros((I * count, rows), F32)
    for i in range(I):
        pick = (col_b == (row_b // (I * items)) * items + lax.rem(row_b, I * items) - i * items) & (
            lax.rem(row_b, I * items) // items == i
        )
        back = back + dot_nn(pick.astype(F32).astype(BF16), down[i])
    back_out[...] = back
    for n in range(1, E):
        spread_expert(back_out, back_in, s_back, r_back, n, "start")
    back_in[pl.ds(pl.multiple_of(e * step8, step8), step8), :] = back_out[pl.ds(pl.multiple_of(e * step8, step8), step8), :]
    turned = pltpu.roll(gate_table, lax.rem(128 - c * (I * 2 * items), 128), 1)
    for n in range(1, E):
        spread_expert(back_out, back_in, s_back, r_back, n, "recv")
    for s in range(E):
        value = jnp.zeros((total, rows), F32)
        for i in range(I):
            for j in range(items):
                line = back_in[s * step8 + i * items + j : s * step8 + i * items + j + 1, :]
                lane = i * 2 * items + j
                value = value + turned[:, lane : lane + 1] * line
        comb[c, s] = value
    for n in range(1, C):
        gather_cache(comb, s_comb, r_comb, n, "start")
    put_together(2)
    for n in range(1, C):
        gather_cache(comb, s_comb, r_comb, n, "recv")
    pieces = []
    for s in range(E):
        value = comb[0, s]
        for m in range(1, C):
            value = value + comb[m, s]
        pieces.append(value)
    mixed_ref[...] = attention + jnp.concatenate(pieces, axis=1)

    for w in range(3):
        for i in range(I):
            for o in range(O):
                hop(w, i, o, "send")
                pass_on(w, o, i, "send")
            for kd in range(NEAR):
                direct(w, i, kd, "send")
    for n in range(1, C):
        part(n, "send")
        gather_cache(proj, s_proj, r_proj, n, "send")
        gather_cache(slots_all, s_slot, r_slot, n, "send")
        gather_cache(comb, s_comb, r_comb, n, "send")
    for n in range(1, E):
        spread_expert(out_slots, in_slots, s_disp, r_disp, n, "send")
        spread_expert(back_out, back_in, s_back, r_back, n, "send")
    for n in range(E):
        hidden(n, "send")


def store_kernel(S, R, g_ref, u_ref, d_ref, mixed_ref, go_hbm, uo_hbm, do_hbm, mo_ref, sems):
    copies = [
        pltpu.make_async_copy(source, target, sems.at[n])
        for n, (source, target) in enumerate(((g_ref, go_hbm), (u_ref, uo_hbm), (d_ref, do_hbm)))
    ]
    for copy in copies:
        copy.start()
    for s in range(S):
        mo_ref[s] = mixed_ref[s * R : (s + 1) * R, :].astype(BF16)
    for copy in copies:
        copy.wait()


def whole_shards(
    queries, k_cache, v_cache, lengths, w_out, norm_gain, w_gate, w_up, w_down, expert_ids, gate_weights
):
    C = lax.axis_size("cache")
    E = lax.axis_size("expert")
    I, rows, hidden_width = w_gate.shape
    width = hidden_width // C
    S, R = queries.shape[0], queries.shape[1]
    positions = k_cache.shape[1]
    d_model = E * rows
    cap = 2
    items = S * cap
    O = C - NEAR
    chunk = 256 * (-(-d_model // (256 * C)))
    shape = jax.ShapeDtypeStruct
    any_spec = pl.BlockSpec(memory_space=pl.ANY)
    vmem = pl.BlockSpec(memory_space=pltpu.VMEM)
    smem = pl.BlockSpec(memory_space=pltpu.SMEM)
    V = pltpu.VMEM
    sem = pltpu.SemaphoreType.DMA
    per_row = QH // KVH * S
    gate, up, down, mixed = pl.pallas_call(
        functools.partial(whole_kernel, C, E, I, S, R, cap),
        out_shape=(
            pltpu.VMEM((width, d_model), BF16),
            pltpu.VMEM((width, d_model), BF16),
            pltpu.VMEM((width, d_model), BF16),
            pltpu.VMEM((S * R, d_model), F32),
        ),
        in_specs=[smem, smem, smem, vmem, vmem] + [any_spec] * 6,
        out_specs=(vmem,) * 4,
        scratch_shapes=[
            V((I, rows, hidden_width), BF16),
            V((I, rows, hidden_width), BF16),
            V((I, C, width, rows), BF16),
            V((I, C, width, rows), BF16),
            V((I, C, width, rows), BF16),
            V((O, I, width, rows), BF16),
            V((O, I, width, rows), BF16),
            V((O, I, width, rows), BF16),
            V((E, width, rows), BF16),
            V((E, width, rows), BF16),
            V((E, width, rows), BF16),
            V(k_cache.shape, BF16),
            V(v_cache.shape, BF16),
            V((d_model, w_out.shape[0]), BF16),
            V((S * R, QH * HD), F32),
            V((C, R * per_row, 128), F32),
            V((C, R * per_row, 128), F32),
            V((C, S * R, d_model), F32),
            V((S * R, C * chunk), F32),
            V((E * 2 * items, chunk // 2), F32),
            V((E * 2 * items, chunk // 2), F32),
            V((8, 128), BF16),
            V((C, E * 2 * items, chunk // 2), BF16),
            V((E * items, C * chunk), BF16),
            V((E * items, width), BF16),
            V((I, C, E * items, width), BF16),
            V((I * E * items, rows), F32),
            V((I * E * items, rows), F32),
            V((C, E, S * R, rows), F32),
            sem((4, 2)),
            sem((3, I, O)),
            sem((3, O, I)),
            sem((3, I, NEAR)),
            sem((3, O, I)),
            sem((3, E)),
            sem((3,)),
            sem((C,)),
            sem((C,)),
            sem((C,)),
            sem((C,)),
            sem((E,)),
            sem((E,)),
            sem((C,)),
            sem((C,)),
            sem((E,)),
            sem((I, C)),
            sem((E,)),
            sem((E,)),
            sem((C,)),
            sem((C,)),
        ],
        compiler_params=pltpu.CompilerParams(
            collective_id=0, has_side_effects=True, vmem_limit_bytes=54 << 20
        ),
    )(
        lengths,
        expert_ids,
        gate_weights,
        queries,
        norm_gain.reshape(1, d_model),
        k_cache,
        v_cache,
        w_out.T,
        w_gate,
        w_up,
        w_down.reshape(I, C, width, rows),
    )
    gate, up, down, mixed = (pltpu.with_memory_space_constraint(a, pltpu.VMEM) for a in (gate, up, down, mixed))
    gate, up, down, mixed = pl.pallas_call(
        functools.partial(store_kernel, S, R),
        out_shape=(
            shape((width, d_model), BF16),
            shape((width, d_model), BF16),
            shape((width, d_model), BF16),
            shape((S, R, d_model), BF16),
        ),
        in_specs=[vmem] * 4,
        out_specs=(any_spec,) * 3 + (vmem,),
        scratch_shapes=[sem((3,))],
        compiler_params=pltpu.CompilerParams(vmem_limit_bytes=2 << 20),
    )(gate, up, down, mixed)
    return (
        mixed,
        gate.T.reshape(1, d_model, width),
        up.T.reshape(1, d_model, width),
        down.reshape(1, width, d_model),
    )


def exchange_plain(w_gate, w_up, w_down):
    gate_owner, up_owner = (
        lax.all_to_all(
            lax.all_to_all(w, "cache", split_axis=2, concat_axis=0, tiled=True),
            "expert",
            split_axis=0,
            concat_axis=1,
            tiled=True,
        )
        for w in (w_gate, w_up)
    )
    down_owner = lax.all_to_all(
        lax.all_to_all(w_down, "cache", split_axis=1, concat_axis=0, tiled=True),
        "expert",
        split_axis=0,
        concat_axis=2,
        tiled=True,
    )
    return gate_owner, up_owner, down_owner


def plain_shards(
    queries,
    k_cache,
    v_cache,
    lengths,
    w_out,
    norm_gain,
    w_gate,
    w_up,
    w_down,
    expert_ids,
    gate_weights,
):
    gate_owner, up_owner, down_owner = exchange_plain(w_gate, w_up, w_down)
    cache_count = lax.axis_size("cache")
    cache_place = lax.axis_index("cache")
    step_count = queries.shape[0]
    row_count = k_cache.shape[0]
    positions = k_cache.shape[1]
    group_size = QH // KVH
    heads = queries.reshape(step_count, row_count, KVH, group_size, HD).transpose(1, 2, 0, 3, 4)
    same = jnp.eye(KVH, dtype=jnp.float32)
    spread = heads[:, :, :, :, None, :] * same.astype(heads.dtype)[None, :, None, None, :, None]
    spread = spread.reshape(row_count, step_count * QH, KVH * HD)
    scores = jnp.einsum(
        "rnk,rpk->rnp", spread, k_cache, preferred_element_type=jnp.float32
    ) * (1.0 / math.sqrt(HD))
    position = cache_place * positions + jnp.arange(positions, dtype=jnp.int32)
    limit = lengths[:, None] + jnp.arange(step_count, dtype=jnp.int32)[None, :] + 1
    limit = jnp.broadcast_to(
        limit[:, None, :, None], (row_count, KVH, step_count, group_size)
    ).reshape(row_count, step_count * QH)
    visible = position[None, None, :] < limit[:, :, None]
    highest = jnp.max(jnp.where(visible, scores, -1e30), axis=-1)
    weights = jnp.where(visible, jnp.exp(scores - highest[..., None]), 0.0)
    mass = jnp.sum(weights, axis=-1)
    accum = jnp.einsum(
        "rnp,rpk->rnk",
        weights.astype(jnp.bfloat16),
        v_cache,
        preferred_element_type=jnp.float32,
    ).reshape(row_count, KVH, step_count, group_size, KVH, HD)
    accum = jnp.sum(accum * same[None, :, None, None, :, None], axis=4)

    def by_step(a):
        return jnp.moveaxis(a, 2, 0).reshape(step_count, row_count, -1)

    accum = by_step(accum)
    highest = by_step(highest.reshape(row_count, KVH, step_count, group_size))
    mass = by_step(mass.reshape(row_count, KVH, step_count, group_size))
    own_width = w_out.shape[0]
    gathered = lax.all_gather(jnp.concatenate((accum, highest, mass), axis=-1), "cache")
    own_heads = own_width // HD
    all_high = gathered[..., QH * HD : QH * HD + QH]
    factor = jnp.exp(all_high - jnp.max(all_high, axis=0))
    all_mass = jnp.sum(gathered[..., QH * HD + QH :] * factor, axis=0)
    own_factor = lax.dynamic_slice_in_dim(factor / all_mass, cache_place * own_heads, own_heads, 3)
    own_accum = lax.dynamic_slice_in_dim(gathered, cache_place * own_width, own_width, 3)
    own_out = jnp.sum(own_accum * jnp.repeat(own_factor, HD, axis=-1), axis=0)
    own_rows = own_out.astype(jnp.bfloat16).reshape(step_count * row_count, own_width)
    projected = jnp.dot(own_rows, w_out, preferred_element_type=jnp.float32)
    attention = jnp.sum(lax.all_gather(projected, "cache"), axis=0)
    scale = lax.rsqrt(jnp.mean(attention * attention, axis=-1, keepdims=True) + 1e-05)
    normed = (attention * scale * norm_gain).astype(jnp.bfloat16).reshape(step_count, row_count, D)
    experts_total = w_gate.shape[0] * cache_count
    capacity = max(2, (row_count * TOP + experts_total - 1) // experts_total)
    expert_range = jnp.arange(experts_total, dtype=jnp.int32)
    onehot = (expert_ids[..., None] == expert_range).astype(jnp.float32)
    chosen = jnp.sum(onehot, axis=2)
    gate_map = jnp.sum(onehot * gate_weights[..., None], axis=2)
    earlier = jnp.tril(jnp.ones((row_count, row_count), jnp.float32), -1)
    ranks = jnp.einsum("rq,sqe->sre", earlier, chosen, precision=lax.Precision.HIGHEST)
    slot_table = (ranks[..., None] == jnp.arange(capacity, dtype=jnp.float32)).astype(
        jnp.float32
    ) * chosen[..., None]
    outgoing = jnp.einsum(
        "srec,srd->escd",
        slot_table.astype(jnp.bfloat16),
        normed,
        preferred_element_type=jnp.float32,
    )
    outgoing = outgoing.astype(jnp.bfloat16).reshape(experts_total, step_count * capacity, D)
    slots = lax.all_to_all(outgoing, "expert", split_axis=0, concat_axis=0, tiled=True)
    source_count = slots.shape[0]
    item_count = slots.shape[1]
    slot_rows = slots.reshape(source_count * item_count, D)
    gate_value = jnp.dot(slot_rows, gate_owner[0], preferred_element_type=jnp.float32)
    up_value = jnp.dot(slot_rows, up_owner[0], preferred_element_type=jnp.float32)
    hidden = (jax.nn.silu(gate_value) * up_value).astype(jnp.bfloat16)
    partial_out = jnp.dot(hidden, down_owner[0], preferred_element_type=jnp.float32).reshape(
        source_count, item_count, D
    )
    expert_out = partial_out.astype(jnp.bfloat16)
    returned = lax.all_to_all(expert_out, "expert", split_axis=0, concat_axis=0, tiled=True)
    back_width = returned.shape[-1]
    returned = returned.reshape(experts_total, step_count, capacity, back_width)
    combined = jnp.einsum(
        "srec,escd->srd",
        slot_table * gate_map[..., None],
        returned.astype(jnp.float32),
        precision=lax.Precision.HIGHEST,
    )
    attention_rows = attention.reshape(step_count, row_count, D)
    combined = jnp.sum(lax.all_gather(combined, "cache"), axis=0)
    mixed = (attention_rows + combined).astype(jnp.bfloat16)
    return (mixed, gate_owner, up_owner, down_owner)


def shards(*args):
    queries, w_out, w_gate = args[0], args[4], args[6]
    C, E = lax.axis_size("cache"), lax.axis_size("expert")
    I, rows, hidden_width = w_gate.shape
    fits = (
        C % NEAR == 0
        and C > NEAR
        and C == KVH
        and I * C == E
        and rows % 8 == 0
        and hidden_width % (8 * C) == 0
        and w_out.shape[0] * C == QH * HD
        and queries.shape[0] * queries.shape[1] == 8
        and I * queries.shape[0] * 2 == 8
        and 2 * queries.shape[0] * 2 == 8
        and queries.shape[1] * TOP <= 2 * E
    )
    return (whole_shards if fits else plain_shards)(*args)


def solution(mesh):
    return jax.shard_map(
        shards,
        mesh=mesh,
        in_specs=(
            P(None, "expert", None),
            P("expert", "cache", None),
            P("expert", "cache", None),
            P("expert"),
            P("cache", None),
            P(),
            P("cache", "expert", None),
            P("cache", "expert", None),
            P("cache", None, "expert"),
            P(None, "expert", None),
            P(None, "expert", None),
        ),
        out_specs=(
            P(None, "expert", None),
            P("expert", None, "cache"),
            P("expert", None, "cache"),
            P("expert", "cache", None),
        ),
        check_vma=False,
    )
```

```python
import functools
import math

import jax
import jax.numpy as jnp
from jax import lax
from jax.experimental import pallas as pl
from jax.experimental.pallas import tpu as pltpu
from jax.sharding import PartitionSpec as P

D = 2880
QH = 32
KVH = 4
HD = 64
TOP = 4
NEAR = 2

MESH = pl.DeviceIdType.MESH
F32 = jnp.float32
BF16 = jnp.bfloat16


def dot_nt(a, b):
    return lax.dot_general(a, b, (((1,), (1,)), ((), ())), preferred_element_type=F32)


def dot_nn(a, b):
    return jnp.dot(a, b, preferred_element_type=F32)


def iota(shape, axis):
    return lax.broadcasted_iota(jnp.int32, shape, axis)


def whole_kernel(
    C, E, I, S, R, cap,
    lengths, ids, gates, q_ref, gain_ref, k_hbm, v_hbm, wo_hbm, wg_hbm, wu_hbm, wd_hbm,
    g_own, u_own, d_own, mixed_ref,
    g_in, u_in, d_in, g_stage, u_stage, d_stage, relay_g, relay_u, relay_d, fin_g, fin_u, fin_d,
    k_in, v_in, wo_in, q_f32, part_out, part_in, proj, normed, out_slots, slots_all,
    rows_x, hid_out, hid_in, back_out, back_in, comb,
    load_sem, sx, r1, sd, sr, rf, loc, s_part, r_part, s_proj, r_proj, s_disp, r_disp, s_slot, r_slot,
    s_hid, r_hid, s_back, r_back, s_comb, r_comb,
):
    c = lax.axis_index("cache")
    e = lax.axis_index("expert")
    x = c // NEAR
    k = lax.rem(c, NEAR)
    O = C - NEAR
    width = g_own.shape[0]
    rows = g_in.shape[1]
    full = rows // 128 * 128
    rest = rows - full
    group = QH // KVH
    per_row = group * S
    heads_rows = KVH * per_row
    items = S * cap
    total = S * R
    half = out_slots.shape[2]
    chunk = half * 2
    d_model = E * rows

    load_k = pltpu.make_async_copy(k_hbm, k_in, load_sem.at[3, 0])
    load_v = pltpu.make_async_copy(v_hbm, v_in, load_sem.at[3, 1])
    load_g = [pltpu.make_async_copy(wg_hbm.at[i], g_in.at[i], load_sem.at[0, i]) for i in range(I)]
    load_u = [pltpu.make_async_copy(wu_hbm.at[i], u_in.at[i], load_sem.at[1, i]) for i in range(I)]
    load_d = pltpu.make_async_copy(wd_hbm, d_in, load_sem.at[2, 0])
    load_wo = pltpu.make_async_copy(wo_hbm, wo_in, load_sem.at[2, 1])
    loads = [load_k, load_v, load_g[0], load_wo] + load_g[1:] + load_u + [load_d]
    for load in loads:
        load.start()

    barrier = pltpu.get_barrier_semaphore()
    me = c * E + e
    for n in range(1, C * E):
        other = lax.rem(me + n, C * E)
        pl.semaphore_signal(barrier, inc=1, device_id=(other // E, lax.rem(other, E)), device_id_type=MESH)

    relays = (relay_g, relay_u, relay_d)
    finals = (fin_g, fin_u, fin_d)

    def remote(src, dst, send, recv, tc, te):
        return pltpu.make_async_remote_copy(
            src_ref=src, dst_ref=dst, send_sem=send, recv_sem=recv, device_id=(tc, te), device_id_type=MESH
        )

    def block(w, i, target):
        return (g_stage, u_stage, d_stage)[w].at[i, target]

    def far(o):
        return lax.rem(x * NEAR + NEAR + o, C)

    def direct(w, i, kd, action):
        target = x * NEAR + kd
        owner = c * I + i
        own = (owner == e) & (k == kd)

        @pl.when(own)
        def _():
            if action == "start":
                pltpu.make_async_copy(block(w, i, target), finals[w].at[e], loc.at[w]).start()

        @pl.when(jnp.logical_not(own))
        def _():
            copy = remote(block(w, i, target), finals[w].at[e], sd.at[w, i, kd], rf.at[w, e], target, owner)
            copy.start() if action == "start" else copy.wait_send()

    def hop(w, i, o, action):
        target = far(o)
        owner = c * I + i
        place = lax.rem(c - (target // NEAR) * NEAR - NEAR + 2 * C, C)

        @pl.when(owner == e)
        def _():
            copy = remote(block(w, i, target), finals[w].at[e], sx.at[w, i, o], rf.at[w, e], target, e)
            copy.start() if action == "start" else copy.wait_send()

        @pl.when(owner != e)
        def _():
            copy = remote(block(w, i, target), relays[w].at[place, i], sx.at[w, i, o], r1.at[w, place, i], target, e)
            copy.start() if action == "start" else copy.wait_send()

    def pass_on(w, o, i, action):
        owner = far(o) * I + i

        @pl.when(owner != e)
        def _():
            part = relays[w].at[o, i]
            copy = remote(part, finals[w].at[e], sr.at[w, o, i], rf.at[w, e], c, owner)
            if action == "start":
                remote(part, part, sr.at[w, o, i], r1.at[w, o, i], c, owner).wait_recv()
                copy.start()
            else:
                copy.wait_send()

    def arrived(w, s):
        own = (c == e // I) & (e == s)

        @pl.when(own)
        def _():
            pltpu.make_async_copy(finals[w].at[s], finals[w].at[s], loc.at[w]).wait()

        @pl.when(jnp.logical_not(own))
        def _():
            remote(finals[w].at[s], finals[w].at[s], sd.at[w, 0, 0], rf.at[w, s], c, s).wait_recv()

    tiles = -(-width // 128)

    def stage(w, i):
        for t in range(C):
            if w < 2:
                part = (g_in, u_in)[w][i, :, t * width : (t + 1) * width]
                main, last = part[:full].T, part[full:]
            else:
                main, last = d_in[i, t, :, :full], d_in[i, t, :, full:].T
            target = (g_stage, u_stage, d_stage)[w]
            for j in range(full // 128):
                target[i, t, j * width : (j + 1) * width, :] = main[:, j * 128 : (j + 1) * 128]
            last = jnp.concatenate([last, jnp.zeros((rest, tiles * 128 - width), BF16)], axis=1)
            base = full // 128 * width
            for j in range(tiles):
                target[i, t, base + j * rest : base + (j + 1) * rest, :] = last[:, j * 128 : (j + 1) * 128]

    def put_together(w):
        own = (g_own, u_own, d_own)[w]
        for s in range(E):
            arrived(w, s)
            for j in range(full // 128):
                at = s * rows + j * 128
                own[:, at : at + 128] = finals[w][s, j * width : (j + 1) * width, :]
            base = full // 128 * width
            last = jnp.concatenate(
                [finals[w][s, base + j * rest : base + (j + 1) * rest, :] for j in range(tiles)], axis=1
            )
            own[:, s * rows + full : (s + 1) * rows] = last[:, :width].T

    def gather_cache(buffer, send, recv, n, action):
        target = lax.rem(c + n, C)
        if action == "recv":
            remote(buffer.at[target], buffer.at[target], send.at[target], recv.at[target], target, e).wait_recv()
            return
        copy = remote(buffer.at[c], buffer.at[c], send.at[target], recv.at[c], target, e)
        copy.start() if action == "start" else copy.wait_send()

    for s in range(S):
        q_f32[s * R : (s + 1) * R, :] = q_ref[s].astype(F32)
    lane_q = iota((heads_rows, QH * HD), 1)
    row_q = iota((heads_rows, QH * HD), 0)
    head_of_row = (row_q // per_row) * group + lax.rem(row_q, per_row) // S
    mine = (lane_q // HD) == head_of_row
    step_q = lax.rem(row_q, S)
    fold_l = iota((QH * HD, KVH * HD), 0)
    fold_m = iota((QH * HD, KVH * HD), 1)
    fold = ((lax.rem(fold_l, HD) == lax.rem(fold_m, HD)) & (fold_l // (group * HD) == fold_m // HD)).astype(F32).astype(BF16)
    load_k.wait()
    load_v.wait()
    positions = k_in.shape[1]
    place_of = c * positions + iota((heads_rows, positions), 1)
    step_p = lax.rem(iota((heads_rows, positions), 0), S)
    lane_t = iota((per_row, 128), 1)
    for r in range(R):
        rows_q = q_f32[r : r + 1, :]
        spread = jnp.broadcast_to(rows_q, (heads_rows, QH * HD))
        for s in range(1, S):
            spread = jnp.where(step_q == s, jnp.broadcast_to(q_f32[s * R + r : s * R + r + 1, :], spread.shape), spread)
        spread = jnp.where(mine, spread, 0.0).astype(BF16)
        spread = dot_nn(spread, fold).astype(BF16)
        score = dot_nt(spread, k_in[r]) * (1.0 / math.sqrt(HD))
        visible = place_of < lengths[r] + step_p + 1
        highest = jnp.max(jnp.where(visible, score, -1e30), axis=1, keepdims=True)
        weight = jnp.where(visible, jnp.exp(score - highest), 0.0)
        mass = jnp.sum(weight, axis=1, keepdims=True)
        accum = dot_nn(weight.astype(BF16), v_in[r])
        for h in range(KVH):
            span = slice(h * per_row, (h + 1) * per_row)
            base = (h * HD // 128) * 128
            piece = accum[span, base : base + 128]
            if h * HD % 128:
                piece = pltpu.roll(piece, 128 - HD, 1)
            piece = jnp.where(lane_t < HD, piece, jnp.where(lane_t < HD + 32, highest[span], mass[span]))
            part_out[h, r * per_row : (r + 1) * per_row, :] = piece

    pl.semaphore_wait(barrier, C * E - 1)

    def part(n, action):
        target = lax.rem(c + n, C)
        if action == "recv":
            remote(part_in.at[target], part_in.at[target], s_part.at[target], r_part.at[target], target, e).wait_recv()
            return
        copy = remote(part_out.at[target], part_in.at[c], s_part.at[target], r_part.at[c], target, e)
        copy.start() if action == "start" else copy.wait_send()

    for n in range(1, C):
        part(n, "start")
    part_in[c] = part_out[c]

    def leave(w, i):
        if w < 2:
            (load_g, load_u)[w][i].wait()
        stage(w, i)
        for o in range(O):
            hop(w, i, o, "start")

    def straight(w, i):
        for kd in range(NEAR):
            direct(w, i, kd, "start")

    def onward(w, i):
        for o in range(O):
            pass_on(w, o, i, "start")

    leave(0, 0)
    straight(0, 0)
    for n in range(1, C):
        part(n, "recv")
    tall = R * per_row
    top = part_in[0][:, HD : HD + 1]
    for s in range(1, C):
        top = jnp.maximum(top, part_in[s][:, HD : HD + 1])
    number = jnp.zeros((tall, 128), F32)
    mass = jnp.zeros((tall, 1), F32)
    for s in range(C):
        one = part_in[s]
        factor = jnp.exp(one[:, HD : HD + 1] - top)
        number = number + one * factor
        mass = mass + one[:, HD + 32 : HD + 33] * factor
    number = number / mass
    lane_h = iota((tall, 128), 1)
    number = jnp.where(lane_h < HD, number, pltpu.roll(number, HD, 1))
    number = jnp.concatenate([number] * (group * HD // 128), axis=1)
    lane_w = iota(number.shape, 1)
    row_w = iota(number.shape, 0)
    number = jnp.where(lane_w // HD == lax.rem(row_w, per_row) // S, number, 0.0).astype(BF16)
    row_s = iota((total, tall), 0)
    col_s = iota((total, tall), 1)
    gather = ((col_s // per_row == lax.rem(row_s, R)) & (lax.rem(col_s, S) == row_s // R)).astype(F32).astype(BF16)
    heads_out = dot_nn(gather, number).astype(BF16)
    load_wo.wait()
    proj[c] = dot_nt(heads_out, wo_in[...])

    for n in range(1, C):
        gather_cache(proj, s_proj, r_proj, n, "start")

    leave(0, 1)
    straight(0, 1)
    leave(1, 0)
    def table(shape, row_axis):
        row = iota(shape, row_axis)
        slot = iota(shape, 1 - row_axis)
        expert = slot // (2 * items)
        inside = lax.rem(slot, items)
        chosen = jnp.zeros(shape, F32)
        weight = jnp.zeros(shape, F32)
        for s in range(S):
            for r in range(R):
                for t in range(TOP):
                    hit = (row == s * R + r) & (expert == ids[s, r, t])
                    chosen = jnp.where(hit, 1.0, chosen)
                    weight = jnp.where(hit, gates[s, r, t], weight)
        rank = jnp.zeros(shape, F32)
        place = lax.rem(row, R)
        for n in range(1, R):
            rank = rank + jnp.where(place >= n, pltpu.roll(chosen, n, row_axis), 0.0)
        fit = (row < total) & (inside // cap == row // R) & (rank == lax.rem(inside, cap).astype(F32))
        chosen = jnp.where(fit, chosen, 0.0)
        return chosen, weight * chosen

    send_table, _ = table((E * 2 * items, 128), 1)
    _, gate_table = table((total, 128), 0)

    onward(0, 0)
    for n in range(1, C):
        gather_cache(proj, s_proj, r_proj, n, "recv")
    attention = proj[0]
    for s in range(1, C):
        attention = attention + proj[s]
    scale = lax.rsqrt(jnp.sum(attention * attention, axis=1, keepdims=True) * (1.0 / d_model) + 1e-05)
    normed[:, d_model:] = jnp.zeros((total, C * chunk - d_model), F32)
    normed[:, :d_model] = (attention * scale * gain_ref[...].reshape(1, d_model)).astype(BF16).astype(F32)
    own_chunk = normed[:, pl.ds(pl.multiple_of(c * chunk, 128), chunk)]
    placed = dot_nn(send_table[:, :total], own_chunk)
    upper = lax.rem(iota((E * 2 * items, half), 0), 2 * items) < items
    out_slots[...] = jnp.where(upper, placed[:, :half], placed[:, half:]).reshape(out_slots.shape).astype(BF16)

    def spread_expert(out, back, send, recv, n, action):
        target = lax.rem(e + n, E)
        if action == "recv":
            spot = back.at[target]
            remote(spot, spot, send.at[target], recv.at[target], c, target).wait_recv()
            return
        copy = remote(out.at[target], back.at[e], send.at[target], recv.at[e], c, target)
        copy.start() if action == "start" else copy.wait_send()

    for n in range(1, E):
        spread_expert(out_slots, slots_all.at[c], s_disp, r_disp, n, "start")
    slots_all[c, e] = out_slots[e]

    straight(1, 0)
    onward(0, 1)
    leave(1, 1)
    load_d.wait()
    leave(2, 0)
    leave(2, 1)
    onward(1, 0)
    straight(1, 1)
    onward(1, 1)
    for n in range(1, E):
        spread_expert(out_slots, slots_all.at[c], s_disp, r_disp, n, "recv")
    for n in range(1, C):
        gather_cache(slots_all, s_slot, r_slot, n, "start")
    straight(2, 0)
    onward(2, 0)
    for n in range(1, C):
        gather_cache(slots_all, s_slot, r_slot, n, "recv")
    count = E * items
    row_t = iota((count, 2 * count), 0)
    col_t = iota((count, 2 * count), 1)
    base = (row_t // items) * (2 * items) + lax.rem(row_t, items)
    take_low = (col_t == base).astype(F32).astype(BF16)
    take_high = (col_t == base + items).astype(F32).astype(BF16)
    for s in range(C):
        slots = slots_all[s].astype(F32).reshape(2 * count, half).astype(BF16)
        rows_x[:, s * chunk : s * chunk + half] = dot_nn(take_low, slots).astype(BF16)
        rows_x[:, s * chunk + half : (s + 1) * chunk] = dot_nn(take_high, slots).astype(BF16)

    put_together(0)
    gate_value = dot_nt(rows_x[:, :d_model], g_own[...])
    put_together(1)
    up_value = dot_nt(rows_x[:, :d_model], u_own[...])
    hid_out[...] = (gate_value * jax.nn.sigmoid(gate_value) * up_value).astype(BF16)

    column = e // I
    inner = lax.rem(e, I)

    def hidden(n, action):
        target = lax.rem(e + n, E)
        own = (column == c) & (target == e)

        @pl.when(jnp.logical_not(own))
        def _():
            copy = remote(hid_out, hid_in.at[inner, c], s_hid.at[target], r_hid.at[inner, c], column, target)
            copy.start() if action == "start" else copy.wait_send()

        if n == 0 and action == "start":

            @pl.when(own)
            def _():
                hid_in[inner, c] = hid_out[...]

    for n in range(E):
        hidden(n, "start")
    direct(2, 1, 0, "start")
    pass_on(2, 0, 1, "start")
    down = []
    for i in range(I):
        value = jnp.zeros((count, rows), F32)
        for s in range(C):
            @pl.when(jnp.logical_not((s == c) & (e == c * I + i)))
            def _():
                remote(hid_in.at[i, s], hid_in.at[i, s], s_hid.at[0], r_hid.at[i, s], s, e).wait_recv()
            value = value + dot_nn(hid_in[i, s], d_in[i, s])
        down.append(value.astype(BF16))
    row_b = iota((I * count, count), 0)
    col_b = iota((I * count, count), 1)
    back = jnp.zeros((I * count, rows), F32)
    for i in range(I):
        pick = (col_b == (row_b // (I * items)) * items + lax.rem(row_b, I * items) - i * items) & (
            lax.rem(row_b, I * items) // items == i
        )
        back = back + dot_nn(pick.astype(F32).astype(BF16), down[i])
    back_out[...] = back.reshape(back_out.shape).astype(BF16)
    for n in range(1, E):
        spread_expert(back_out, back_in, s_back, r_back, n, "start")
    direct(2, 1, 1, "start")
    pass_on(2, 1, 1, "start")
    back_in[e] = back_out[e]
    turned = pltpu.roll(gate_table, lax.rem(128 - c * (I * 2 * items), 128), 1)
    for n in range(1, E):
        spread_expert(back_out, back_in, s_back, r_back, n, "recv")
    for s in range(E):
        value = jnp.zeros((total, rows), F32)
        given = back_in[s].astype(F32)
        for i in range(I):
            for j in range(items):
                lane = i * 2 * items + j
                value = value + turned[:, lane : lane + 1] * given[i * items + j : i * items + j + 1, :]
        comb[c, s] = value.astype(BF16)
    for n in range(1, C):
        gather_cache(comb, s_comb, r_comb, n, "start")
    put_together(2)
    for n in range(1, C):
        gather_cache(comb, s_comb, r_comb, n, "recv")
    pieces = []
    for s in range(E):
        value = comb[0, s].astype(F32)
        for m in range(1, C):
            value = value + comb[m, s].astype(F32)
        pieces.append(value)
    mixed_ref[...] = attention + jnp.concatenate(pieces, axis=1)

    for w in range(3):
        for i in range(I):
            for o in range(O):
                hop(w, i, o, "send")
                pass_on(w, o, i, "send")
            for kd in range(NEAR):
                direct(w, i, kd, "send")
    for n in range(1, C):
        part(n, "send")
        gather_cache(proj, s_proj, r_proj, n, "send")
        gather_cache(slots_all, s_slot, r_slot, n, "send")
        gather_cache(comb, s_comb, r_comb, n, "send")
    for n in range(1, E):
        spread_expert(out_slots, slots_all.at[c], s_disp, r_disp, n, "send")
        spread_expert(back_out, back_in, s_back, r_back, n, "send")
    for n in range(E):
        hidden(n, "send")


def store_kernel(S, R, g_ref, u_ref, d_ref, mixed_ref, go_hbm, uo_hbm, do_hbm, mo_ref, sems):
    copies = [
        pltpu.make_async_copy(source, target, sems.at[n])
        for n, (source, target) in enumerate(((g_ref, go_hbm), (u_ref, uo_hbm), (d_ref, do_hbm)))
    ]
    for copy in copies:
        copy.start()
    for s in range(S):
        mo_ref[s] = mixed_ref[s * R : (s + 1) * R, :].astype(BF16)
    for copy in copies:
        copy.wait()


def whole_shards(
    queries, k_cache, v_cache, lengths, w_out, norm_gain, w_gate, w_up, w_down, expert_ids, gate_weights
):
    C = lax.axis_size("cache")
    E = lax.axis_size("expert")
    I, rows, hidden_width = w_gate.shape
    width = hidden_width // C
    S, R = queries.shape[0], queries.shape[1]
    positions = k_cache.shape[1]
    d_model = E * rows
    cap = 2
    items = S * cap
    O = C - NEAR
    chunk = 256 * (-(-d_model // (256 * C)))
    shape = jax.ShapeDtypeStruct
    any_spec = pl.BlockSpec(memory_space=pl.ANY)
    vmem = pl.BlockSpec(memory_space=pltpu.VMEM)
    smem = pl.BlockSpec(memory_space=pltpu.SMEM)
    V = pltpu.VMEM
    sem = pltpu.SemaphoreType.DMA
    per_row = QH // KVH * S
    lines = rows // 128 * width + -(-width // 128) * (rows % 128)
    gate, up, down, mixed = pl.pallas_call(
        functools.partial(whole_kernel, C, E, I, S, R, cap),
        out_shape=(
            pltpu.VMEM((width, d_model), BF16),
            pltpu.VMEM((width, d_model), BF16),
            pltpu.VMEM((width, d_model), BF16),
            pltpu.VMEM((S * R, d_model), F32),
        ),
        in_specs=[smem, smem, smem, vmem, vmem] + [any_spec] * 6,
        out_specs=(vmem,) * 4,
        scratch_shapes=[
            V((I, rows, hidden_width), BF16),
            V((I, rows, hidden_width), BF16),
            V((I, C, width, rows), BF16),
            V((I, C, lines, 128), BF16),
            V((I, C, lines, 128), BF16),
            V((I, C, lines, 128), BF16),
            V((O, I, lines, 128), BF16),
            V((O, I, lines, 128), BF16),
            V((O, I, lines, 128), BF16),
            V((E, lines, 128), BF16),
            V((E, lines, 128), BF16),
            V((E, lines, 128), BF16),
            V(k_cache.shape, BF16),
            V(v_cache.shape, BF16),
            V((d_model, w_out.shape[0]), BF16),
            V((S * R, QH * HD), F32),
            V((C, R * per_row, 128), F32),
            V((C, R * per_row, 128), F32),
            V((C, S * R, d_model), F32),
            V((S * R, C * chunk), F32),
            V((E, 2 * items, chunk // 2), BF16),
            V((C, E, 2 * items, chunk // 2), BF16),
            V((E * items, C * chunk), BF16),
            V((E * items, width), BF16),
            V((I, C, E * items, width), BF16),
            V((E, I * items, rows), BF16),
            V((E, I * items, rows), BF16),
            V((C, E, S * R, rows), BF16),
            sem((4, 2)),
            sem((3, I, O)),
            sem((3, O, I)),
            sem((3, I, NEAR)),
            sem((3, O, I)),
            sem((3, E)),
            sem((3,)),
            sem((C,)),
            sem((C,)),
            sem((C,)),
            sem((C,)),
            sem((E,)),
            sem((E,)),
            sem((C,)),
            sem((C,)),
            sem((E,)),
            sem((I, C)),
            sem((E,)),
            sem((E,)),
            sem((C,)),
            sem((C,)),
        ],
        compiler_params=pltpu.CompilerParams(
            collective_id=0, has_side_effects=True, vmem_limit_bytes=54 << 20
        ),
    )(
        lengths,
        expert_ids,
        gate_weights,
        queries,
        norm_gain,
        k_cache,
        v_cache,
        w_out.T,
        w_gate,
        w_up,
        w_down.reshape(I, C, width, rows),
    )
    gate, up, down, mixed = (pltpu.with_memory_space_constraint(a, pltpu.VMEM) for a in (gate, up, down, mixed))
    gate, up, down, mixed = pl.pallas_call(
        functools.partial(store_kernel, S, R),
        out_shape=(
            shape((width, d_model), BF16),
            shape((width, d_model), BF16),
            shape((width, d_model), BF16),
            shape((S, R, d_model), BF16),
        ),
        in_specs=[vmem] * 4,
        out_specs=(any_spec,) * 3 + (vmem,),
        scratch_shapes=[sem((3,))],
        compiler_params=pltpu.CompilerParams(vmem_limit_bytes=2 << 20),
    )(gate, up, down, mixed)
    return (
        mixed,
        gate.T.reshape(1, d_model, width),
        up.T.reshape(1, d_model, width),
        down.reshape(1, width, d_model),
    )


def exchange_plain(w_gate, w_up, w_down):
    gate_owner, up_owner = (
        lax.all_to_all(
            lax.all_to_all(w, "cache", split_axis=2, concat_axis=0, tiled=True),
            "expert",
            split_axis=0,
            concat_axis=1,
            tiled=True,
        )
        for w in (w_gate, w_up)
    )
    down_owner = lax.all_to_all(
        lax.all_to_all(w_down, "cache", split_axis=1, concat_axis=0, tiled=True),
        "expert",
        split_axis=0,
        concat_axis=2,
        tiled=True,
    )
    return gate_owner, up_owner, down_owner


def plain_shards(
    queries,
    k_cache,
    v_cache,
    lengths,
    w_out,
    norm_gain,
    w_gate,
    w_up,
    w_down,
    expert_ids,
    gate_weights,
):
    gate_owner, up_owner, down_owner = exchange_plain(w_gate, w_up, w_down)
    cache_count = lax.axis_size("cache")
    cache_place = lax.axis_index("cache")
    step_count = queries.shape[0]
    row_count = k_cache.shape[0]
    positions = k_cache.shape[1]
    group_size = QH // KVH
    heads = queries.reshape(step_count, row_count, KVH, group_size, HD).transpose(1, 2, 0, 3, 4)
    same = jnp.eye(KVH, dtype=jnp.float32)
    spread = heads[:, :, :, :, None, :] * same.astype(heads.dtype)[None, :, None, None, :, None]
    spread = spread.reshape(row_count, step_count * QH, KVH * HD)
    scores = jnp.einsum(
        "rnk,rpk->rnp", spread, k_cache, preferred_element_type=jnp.float32
    ) * (1.0 / math.sqrt(HD))
    position = cache_place * positions + jnp.arange(positions, dtype=jnp.int32)
    limit = lengths[:, None] + jnp.arange(step_count, dtype=jnp.int32)[None, :] + 1
    limit = jnp.broadcast_to(
        limit[:, None, :, None], (row_count, KVH, step_count, group_size)
    ).reshape(row_count, step_count * QH)
    visible = position[None, None, :] < limit[:, :, None]
    highest = jnp.max(jnp.where(visible, scores, -1e30), axis=-1)
    weights = jnp.where(visible, jnp.exp(scores - highest[..., None]), 0.0)
    mass = jnp.sum(weights, axis=-1)
    accum = jnp.einsum(
        "rnp,rpk->rnk",
        weights.astype(jnp.bfloat16),
        v_cache,
        preferred_element_type=jnp.float32,
    ).reshape(row_count, KVH, step_count, group_size, KVH, HD)
    accum = jnp.sum(accum * same[None, :, None, None, :, None], axis=4)

    def by_step(a):
        return jnp.moveaxis(a, 2, 0).reshape(step_count, row_count, -1)

    accum = by_step(accum)
    highest = by_step(highest.reshape(row_count, KVH, step_count, group_size))
    mass = by_step(mass.reshape(row_count, KVH, step_count, group_size))
    own_width = w_out.shape[0]
    gathered = lax.all_gather(jnp.concatenate((accum, highest, mass), axis=-1), "cache")
    own_heads = own_width // HD
    all_high = gathered[..., QH * HD : QH * HD + QH]
    factor = jnp.exp(all_high - jnp.max(all_high, axis=0))
    all_mass = jnp.sum(gathered[..., QH * HD + QH :] * factor, axis=0)
    own_factor = lax.dynamic_slice_in_dim(factor / all_mass, cache_place * own_heads, own_heads, 3)
    own_accum = lax.dynamic_slice_in_dim(gathered, cache_place * own_width, own_width, 3)
    own_out = jnp.sum(own_accum * jnp.repeat(own_factor, HD, axis=-1), axis=0)
    own_rows = own_out.astype(jnp.bfloat16).reshape(step_count * row_count, own_width)
    projected = jnp.dot(own_rows, w_out, preferred_element_type=jnp.float32)
    attention = jnp.sum(lax.all_gather(projected, "cache"), axis=0)
    scale = lax.rsqrt(jnp.mean(attention * attention, axis=-1, keepdims=True) + 1e-05)
    normed = (attention * scale * norm_gain).astype(jnp.bfloat16).reshape(step_count, row_count, D)
    experts_total = w_gate.shape[0] * cache_count
    capacity = max(2, (row_count * TOP + experts_total - 1) // experts_total)
    expert_range = jnp.arange(experts_total, dtype=jnp.int32)
    onehot = (expert_ids[..., None] == expert_range).astype(jnp.float32)
    chosen = jnp.sum(onehot, axis=2)
    gate_map = jnp.sum(onehot * gate_weights[..., None], axis=2)
    earlier = jnp.tril(jnp.ones((row_count, row_count), jnp.float32), -1)
    ranks = jnp.einsum("rq,sqe->sre", earlier, chosen, precision=lax.Precision.HIGHEST)
    slot_table = (ranks[..., None] == jnp.arange(capacity, dtype=jnp.float32)).astype(
        jnp.float32
    ) * chosen[..., None]
    outgoing = jnp.einsum(
        "srec,srd->escd",
        slot_table.astype(jnp.bfloat16),
        normed,
        preferred_element_type=jnp.float32,
    )
    outgoing = outgoing.astype(jnp.bfloat16).reshape(experts_total, step_count * capacity, D)
    slots = lax.all_to_all(outgoing, "expert", split_axis=0, concat_axis=0, tiled=True)
    source_count = slots.shape[0]
    item_count = slots.shape[1]
    slot_rows = slots.reshape(source_count * item_count, D)
    gate_value = jnp.dot(slot_rows, gate_owner[0], preferred_element_type=jnp.float32)
    up_value = jnp.dot(slot_rows, up_owner[0], preferred_element_type=jnp.float32)
    hidden = (jax.nn.silu(gate_value) * up_value).astype(jnp.bfloat16)
    partial_out = jnp.dot(hidden, down_owner[0], preferred_element_type=jnp.float32).reshape(
        source_count, item_count, D
    )
    expert_out = partial_out.astype(jnp.bfloat16)
    returned = lax.all_to_all(expert_out, "expert", split_axis=0, concat_axis=0, tiled=True)
    back_width = returned.shape[-1]
    returned = returned.reshape(experts_total, step_count, capacity, back_width)
    combined = jnp.einsum(
        "srec,escd->srd",
        slot_table * gate_map[..., None],
        returned.astype(jnp.float32),
        precision=lax.Precision.HIGHEST,
    )
    attention_rows = attention.reshape(step_count, row_count, D)
    combined = jnp.sum(lax.all_gather(combined, "cache"), axis=0)
    mixed = (attention_rows + combined).astype(jnp.bfloat16)
    return (mixed, gate_owner, up_owner, down_owner)


def shards(*args):
    queries, w_out, w_gate = args[0], args[4], args[6]
    C, E = lax.axis_size("cache"), lax.axis_size("expert")
    I, rows, hidden_width = w_gate.shape
    fits = (
        C % NEAR == 0
        and C > NEAR
        and C == KVH
        and I * C == E
        and rows % 8 == 0
        and rows % 128 > 0
        and rows > 128
        and hidden_width % (8 * C) == 0
        and w_out.shape[0] * C == QH * HD
        and queries.shape[0] * queries.shape[1] == 8
        and I * queries.shape[0] * 2 == 8
        and 2 * queries.shape[0] * 2 == 8
        and queries.shape[1] * TOP <= 2 * E
    )
    return (whole_shards if fits else plain_shards)(*args)


def solution(mesh):
    return jax.shard_map(
        shards,
        mesh=mesh,
        in_specs=(
            P(None, "expert", None),
            P("expert", "cache", None),
            P("expert", "cache", None),
            P("expert"),
            P("cache", None),
            P(),
            P("cache", "expert", None),
            P("cache", "expert", None),
            P("cache", None, "expert"),
            P(None, "expert", None),
            P(None, "expert", None),
        ),
        out_specs=(
            P(None, "expert", None),
            P("expert", None, "cache"),
            P("expert", None, "cache"),
            P("expert", "cache", None),
        ),
        check_vma=False,
    )
```

```python
import functools
import math

import jax
import jax.numpy as jnp
from jax import lax
from jax.experimental import pallas as pl
from jax.experimental.pallas import tpu as pltpu
from jax.sharding import PartitionSpec as P

D = 2880
QH = 32
KVH = 4
HD = 64
TOP = 4
NEAR = 2

MESH = pl.DeviceIdType.MESH
F32 = jnp.float32
BF16 = jnp.bfloat16


def dot_nt(a, b):
    return lax.dot_general(a, b, (((1,), (1,)), ((), ())), preferred_element_type=F32)


def dot_nn(a, b):
    return jnp.dot(a, b, preferred_element_type=F32)


def iota(shape, axis):
    return lax.broadcasted_iota(jnp.int32, shape, axis)


def whole_kernel(
    C, E, I, S, R, cap,
    lengths, ids, gates, q_hbm, gain_hbm, k_hbm, v_hbm, wo_hbm, wg_hbm, wu_hbm, wd_hbm,
    g_own, u_own, d_own, mixed_ref,
    g_in, u_in, d_in, g_stage, u_stage, d_stage, relay_g, relay_u, relay_d, fin_g, fin_u, fin_d,
    k_in, v_in, wo_in, q_ref, gain_ref, q_f32, part_out, part_in, proj, normed, out_slots, slots_all,
    rows_x, hid_out, hid_in, back_out, back_in, comb,
    load_sem, row_sem, sx, r1, r2, sd, sr, rf, loc, s_part, r_part, s_proj, r_proj, s_disp, r_disp, s_slot, r_slot,
    s_hid, r_hid, s_back, r_back, s_comb, r_comb,
):
    c = lax.axis_index("cache")
    e = lax.axis_index("expert")
    x = c // NEAR
    k = lax.rem(c, NEAR)
    O = C - NEAR
    width = g_own.shape[0]
    rows = g_in.shape[1]
    full = rows // 128 * 128
    rest = rows - full
    group = QH // KVH
    per_row = group * S
    heads_rows = KVH * per_row
    items = S * cap
    total = S * R
    half = out_slots.shape[2]
    chunk = half * 2
    d_model = E * rows

    load_q = pltpu.make_async_copy(q_hbm, q_ref, load_sem.at[3, 0])
    load_gain = pltpu.make_async_copy(gain_hbm, gain_ref, load_sem.at[3, 1])
    load_k = [pltpu.make_async_copy(k_hbm.at[r], k_in.at[r], row_sem.at[0, r]) for r in range(R)]
    load_v = [pltpu.make_async_copy(v_hbm.at[r], v_in.at[r], row_sem.at[1, r]) for r in range(R)]
    load_g = [pltpu.make_async_copy(wg_hbm.at[i], g_in.at[i], load_sem.at[0, i]) for i in range(I)]
    load_u = [pltpu.make_async_copy(wu_hbm.at[i], u_in.at[i], load_sem.at[1, i]) for i in range(I)]
    load_d = pltpu.make_async_copy(wd_hbm, d_in, load_sem.at[2, 0])
    load_wo = pltpu.make_async_copy(wo_hbm, wo_in, load_sem.at[2, 1])
    loads = [load_q] + [load for pair in zip(load_k, load_v) for load in pair] + [load_g[0], load_wo, load_gain] + load_g[1:] + load_u + [load_d]
    for load in loads:
        load.start()

    barrier = pltpu.get_barrier_semaphore()
    me = c * E + e
    for n in range(1, C * E):
        other = lax.rem(me + n, C * E)
        pl.semaphore_signal(barrier, inc=1, device_id=(other // E, lax.rem(other, E)), device_id_type=MESH)

    relays = (relay_g, relay_u, relay_d)
    finals = (fin_g, fin_u, fin_d)

    def remote(src, dst, send, recv, tc, te):
        return pltpu.make_async_remote_copy(
            src_ref=src, dst_ref=dst, send_sem=send, recv_sem=recv, device_id=(tc, te), device_id_type=MESH
        )

    def block(w, i, target):
        return (g_stage, u_stage, d_stage)[w].at[i, target]

    lines = g_stage.shape[2]
    parts = (pl.ds(0, lines // 16 * 8), pl.ds(lines // 16 * 8, lines - lines // 16 * 8))

    def far(o):
        return lax.rem(x * NEAR + NEAR + o, C)

    def direct(w, i, kd, action):
        target = x * NEAR + kd
        owner = c * I + i
        own = (owner == e) & (k == kd)

        @pl.when(own)
        def _():
            if action == "start":
                pltpu.make_async_copy(block(w, i, target), finals[w].at[e], loc.at[w]).start()

        @pl.when(jnp.logical_not(own))
        def _():
            copy = remote(block(w, i, target), finals[w].at[e], sd.at[w, i, kd], rf.at[w, e], target, owner)
            copy.start() if action == "start" else copy.wait_send()

    last = (2, I - 1, O - 1)

    def around(source):
        here = e // I
        crossing = (here < C // 2) != (source < C // 2)
        return crossing & (jnp.abs(here - source) == 1)

    def send_around():
        w, i, o = last
        target = far(o)

        @pl.when(around(c))
        def _():
            remote(block(w, i, target), finals[w].at[e], sx.at[w, i, o], rf.at[w, e], target, c * I + i).start()

    def hop(w, i, o, action):
        target = far(o)
        owner = c * I + i
        place = lax.rem(c - (target // NEAR) * NEAR - NEAR + 2 * C, C)

        @pl.when(owner == e)
        def _():
            copy = remote(block(w, i, target), finals[w].at[e], sx.at[w, i, o], rf.at[w, e], target, e)
            copy.start() if action == "start" else copy.wait_send()

        away = owner != e
        if action == "start" and (w, i, o) == last:
            away = away & jnp.logical_not(around(c))

        @pl.when(away)
        def _():
            if action == "send" or (w, i) != (0, 0):
                copy = remote(block(w, i, target), relays[w].at[place, i], sx.at[w, i, o], r1.at[w, place, i], target, e)
                copy.start() if action == "start" else copy.wait_send()
            else:
                for part, arrival in zip(parts, (r1.at[w, place, i], r2.at[place])):
                    remote(
                        block(w, i, target).at[part], relays[w].at[place, i, part], sx.at[w, i, o], arrival, target, e
                    ).start()

    def pass_on(w, o, i, action):
        owner = far(o) * I + i

        away = owner != e
        if (w, i) == last[:2]:
            away = away & jnp.logical_not(around(far(o)) & (k == NEAR - 1))

        @pl.when(away)
        def _():
            part = relays[w].at[o, i]
            if action == "start" and (w, i) == (0, 0):
                for span, arrival in zip(parts, (r1.at[w, o, i], r2.at[o])):
                    half = relays[w].at[o, i, span]
                    remote(half, half, sr.at[w, o, i], arrival, c, owner).wait_recv()
                    remote(half, finals[w].at[e, span], sr.at[w, o, i], rf.at[w, e], c, owner).start()
            elif action == "start":
                remote(part, part, sr.at[w, o, i], r1.at[w, o, i], c, owner).wait_recv()
                remote(part, finals[w].at[e], sr.at[w, o, i], rf.at[w, e], c, owner).start()
            else:
                remote(part, finals[w].at[e], sr.at[w, o, i], rf.at[w, e], c, owner).wait_send()

    def arrived(w, s):
        own = (c == e // I) & (e == s)

        @pl.when(own)
        def _():
            pltpu.make_async_copy(finals[w].at[s], finals[w].at[s], loc.at[w]).wait()

        @pl.when(jnp.logical_not(own))
        def _():
            remote(finals[w].at[s], finals[w].at[s], sd.at[w, 0, 0], rf.at[w, s], c, s).wait_recv()

    tiles = -(-width // 128)

    def stage(w, i):
        for t in range(C):
            if w < 2:
                part = (g_in, u_in)[w][i, :, t * width : (t + 1) * width]
                main, last = part[:full].T, part[full:]
            else:
                main, last = d_in[i, t, :, :full], d_in[i, t, :, full:].T
            target = (g_stage, u_stage, d_stage)[w]
            for j in range(full // 128):
                target[i, t, j * width : (j + 1) * width, :] = main[:, j * 128 : (j + 1) * 128]
            last = jnp.concatenate([last, jnp.zeros((rest, tiles * 128 - width), BF16)], axis=1)
            base = full // 128 * width
            for j in range(tiles):
                target[i, t, base + j * rest : base + (j + 1) * rest, :] = last[:, j * 128 : (j + 1) * 128]

    def put_together(w):
        own = (g_own, u_own, d_own)[w]
        for s in range(E):
            arrived(w, s)
            for j in range(full // 128):
                at = s * rows + j * 128
                own[:, at : at + 128] = finals[w][s, j * width : (j + 1) * width, :]
            base = full // 128 * width
            last = jnp.concatenate(
                [finals[w][s, base + j * rest : base + (j + 1) * rest, :] for j in range(tiles)], axis=1
            )
            own[:, s * rows + full : (s + 1) * rows] = last[:, :width].T

    def gather_cache(buffer, send, recv, n, action):
        target = lax.rem(c + n, C)
        if action == "recv":
            remote(buffer.at[target], buffer.at[target], send.at[target], recv.at[target], target, e).wait_recv()
            return
        copy = remote(buffer.at[c], buffer.at[c], send.at[target], recv.at[c], target, e)
        copy.start() if action == "start" else copy.wait_send()

    lane_q = iota((heads_rows, QH * HD), 1)
    row_q = iota((heads_rows, QH * HD), 0)
    head_of_row = (row_q // per_row) * group + lax.rem(row_q, per_row) // S
    mine = (lane_q // HD) == head_of_row
    step_q = lax.rem(row_q, S)
    fold_l = iota((QH * HD, KVH * HD), 0)
    fold_m = iota((QH * HD, KVH * HD), 1)
    fold = ((lax.rem(fold_l, HD) == lax.rem(fold_m, HD)) & (fold_l // (group * HD) == fold_m // HD)).astype(F32).astype(BF16)
    load_q.wait()
    for s in range(S):
        q_f32[s * R : (s + 1) * R, :] = q_ref[s].astype(F32)
    positions = k_in.shape[1]
    place_of = c * positions + iota((heads_rows, positions), 1)
    step_p = lax.rem(iota((heads_rows, positions), 0), S)
    lane_t = iota((per_row, 128), 1)
    for r in range(R):
        rows_q = q_f32[r : r + 1, :]
        spread = jnp.broadcast_to(rows_q, (heads_rows, QH * HD))
        for s in range(1, S):
            spread = jnp.where(step_q == s, jnp.broadcast_to(q_f32[s * R + r : s * R + r + 1, :], spread.shape), spread)
        spread = jnp.where(mine, spread, 0.0).astype(BF16)
        spread = dot_nn(spread, fold).astype(BF16)
        load_k[r].wait()
        score = dot_nt(spread, k_in[r]) * (1.0 / math.sqrt(HD))
        visible = place_of < lengths[r] + step_p + 1
        highest = jnp.max(jnp.where(visible, score, -1e30), axis=1, keepdims=True)
        weight = jnp.where(visible, jnp.exp(score - highest), 0.0)
        mass = jnp.sum(weight, axis=1, keepdims=True)
        load_v[r].wait()
        accum = dot_nn(weight.astype(BF16), v_in[r])
        for h in range(KVH):
            span = slice(h * per_row, (h + 1) * per_row)
            base = (h * HD // 128) * 128
            piece = accum[span, base : base + 128]
            if h * HD % 128:
                piece = pltpu.roll(piece, 128 - HD, 1)
            piece = jnp.where(lane_t < HD, piece, jnp.where(lane_t < HD + 32, highest[span], mass[span]))
            part_out[h, r * per_row : (r + 1) * per_row, :] = piece

    pl.semaphore_wait(barrier, C * E - 1)

    def part(n, action):
        target = lax.rem(c + n, C)
        if action == "recv":
            remote(part_in.at[target], part_in.at[target], s_part.at[target], r_part.at[target], target, e).wait_recv()
            return
        copy = remote(part_out.at[target], part_in.at[c], s_part.at[target], r_part.at[c], target, e)
        copy.start() if action == "start" else copy.wait_send()

    for n in range(1, C):
        part(n, "start")
    part_in[c] = part_out[c]

    def leave(w, i):
        if w < 2:
            (load_g, load_u)[w][i].wait()
        stage(w, i)
        for o in range(O):
            hop(w, i, o, "start")

    def straight(w, i):
        for kd in range(NEAR):
            direct(w, i, kd, "start")

    def onward(w, i):
        for o in range(O):
            pass_on(w, o, i, "start")

    leave(0, 0)
    straight(0, 0)
    for n in range(1, C):
        part(n, "recv")
    tall = R * per_row
    top = part_in[0][:, HD : HD + 1]
    for s in range(1, C):
        top = jnp.maximum(top, part_in[s][:, HD : HD + 1])
    number = jnp.zeros((tall, 128), F32)
    mass = jnp.zeros((tall, 1), F32)
    for s in range(C):
        one = part_in[s]
        factor = jnp.exp(one[:, HD : HD + 1] - top)
        number = number + one * factor
        mass = mass + one[:, HD + 32 : HD + 33] * factor
    number = number / mass
    lane_h = iota((tall, 128), 1)
    number = jnp.where(lane_h < HD, number, pltpu.roll(number, HD, 1))
    number = jnp.concatenate([number] * (group * HD // 128), axis=1)
    lane_w = iota(number.shape, 1)
    row_w = iota(number.shape, 0)
    number = jnp.where(lane_w // HD == lax.rem(row_w, per_row) // S, number, 0.0).astype(BF16)
    row_s = iota((total, tall), 0)
    col_s = iota((total, tall), 1)
    gather = ((col_s // per_row == lax.rem(row_s, R)) & (lax.rem(col_s, S) == row_s // R)).astype(F32).astype(BF16)
    heads_out = dot_nn(gather, number).astype(BF16)
    load_wo.wait()
    proj[c] = dot_nt(heads_out, wo_in[...])

    for n in range(1, C):
        gather_cache(proj, s_proj, r_proj, n, "start")

    leave(0, 1)
    straight(0, 1)
    leave(1, 0)
    def table(shape, row_axis):
        row = iota(shape, row_axis)
        slot = iota(shape, 1 - row_axis)
        expert = slot // (2 * items)
        inside = lax.rem(slot, items)
        chosen = jnp.zeros(shape, F32)
        weight = jnp.zeros(shape, F32)
        for s in range(S):
            for r in range(R):
                for t in range(TOP):
                    hit = (row == s * R + r) & (expert == ids[s, r, t])
                    chosen = jnp.where(hit, 1.0, chosen)
                    weight = jnp.where(hit, gates[s, r, t], weight)
        rank = jnp.zeros(shape, F32)
        place = lax.rem(row, R)
        for n in range(1, R):
            rank = rank + jnp.where(place >= n, pltpu.roll(chosen, n, row_axis), 0.0)
        fit = (row < total) & (inside // cap == row // R) & (rank == lax.rem(inside, cap).astype(F32))
        chosen = jnp.where(fit, chosen, 0.0)
        return chosen, weight * chosen

    send_table, _ = table((E * 2 * items, 128), 1)
    _, gate_table = table((total, 128), 0)

    onward(0, 0)
    for n in range(1, C):
        gather_cache(proj, s_proj, r_proj, n, "recv")
    attention = proj[0]
    for s in range(1, C):
        attention = attention + proj[s]
    scale = lax.rsqrt(jnp.sum(attention * attention, axis=1, keepdims=True) * (1.0 / d_model) + 1e-05)
    load_gain.wait()
    normed[:, d_model:] = jnp.zeros((total, C * chunk - d_model), F32)
    normed[:, :d_model] = (attention * scale * gain_ref[...].reshape(1, d_model)).astype(BF16).astype(F32)
    own_chunk = normed[:, pl.ds(pl.multiple_of(c * chunk, 128), chunk)]
    placed = dot_nn(send_table[:, :total], own_chunk)
    upper = lax.rem(iota((E * 2 * items, half), 0), 2 * items) < items
    out_slots[...] = jnp.where(upper, placed[:, :half], placed[:, half:]).reshape(out_slots.shape).astype(BF16)

    def spread_expert(out, back, send, recv, n, action):
        target = lax.rem(e + n, E)
        if action == "recv":
            spot = back.at[target]
            remote(spot, spot, send.at[target], recv.at[target], c, target).wait_recv()
            return
        copy = remote(out.at[target], back.at[e], send.at[target], recv.at[e], c, target)
        copy.start() if action == "start" else copy.wait_send()

    for n in range(1, E):
        spread_expert(out_slots, slots_all.at[c], s_disp, r_disp, n, "start")
    slots_all[c, e] = out_slots[e]

    straight(1, 0)
    onward(0, 1)
    leave(1, 1)
    load_d.wait()
    leave(2, 0)
    leave(2, 1)
    onward(1, 0)
    straight(1, 1)
    onward(1, 1)
    for n in range(1, E):
        spread_expert(out_slots, slots_all.at[c], s_disp, r_disp, n, "recv")
    for n in range(1, C):
        gather_cache(slots_all, s_slot, r_slot, n, "start")
    straight(2, 0)
    onward(2, 0)
    direct(2, 1, 0, "start")
    for n in range(1, C):
        gather_cache(slots_all, s_slot, r_slot, n, "recv")
    count = E * items
    row_t = iota((count, 2 * count), 0)
    col_t = iota((count, 2 * count), 1)
    base = (row_t // items) * (2 * items) + lax.rem(row_t, items)
    take_low = (col_t == base).astype(F32).astype(BF16)
    take_high = (col_t == base + items).astype(F32).astype(BF16)
    for s in range(C):
        slots = slots_all[s].astype(F32).reshape(2 * count, half).astype(BF16)
        rows_x[:, s * chunk : s * chunk + half] = dot_nn(take_low, slots).astype(BF16)
        rows_x[:, s * chunk + half : (s + 1) * chunk] = dot_nn(take_high, slots).astype(BF16)

    put_together(0)
    gate_value = dot_nt(rows_x[:, :d_model], g_own[...])
    put_together(1)
    up_value = dot_nt(rows_x[:, :d_model], u_own[...])
    hid_out[...] = (gate_value * jax.nn.sigmoid(gate_value) * up_value).astype(BF16)

    column = e // I
    inner = lax.rem(e, I)

    def hidden(n, action):
        target = lax.rem(e + n, E)
        own = (column == c) & (target == e)

        @pl.when(jnp.logical_not(own))
        def _():
            copy = remote(hid_out, hid_in.at[inner, c], s_hid.at[target], r_hid.at[inner, c], column, target)
            copy.start() if action == "start" else copy.wait_send()

        if n == 0 and action == "start":

            @pl.when(own)
            def _():
                hid_in[inner, c] = hid_out[...]

    for n in range(E):
        hidden(n, "start")
    direct(2, 1, 1, "start")
    send_around()
    pass_on(2, 0, 1, "start")
    down = []
    for i in range(I):
        value = jnp.zeros((count, rows), F32)
        for s in range(C):
            @pl.when(jnp.logical_not((s == c) & (e == c * I + i)))
            def _():
                remote(hid_in.at[i, s], hid_in.at[i, s], s_hid.at[0], r_hid.at[i, s], s, e).wait_recv()
            value = value + dot_nn(hid_in[i, s], d_in[i, s])
        down.append(value.astype(BF16))
    row_b = iota((I * count, count), 0)
    col_b = iota((I * count, count), 1)
    back = jnp.zeros((I * count, rows), F32)
    for i in range(I):
        pick = (col_b == (row_b // (I * items)) * items + lax.rem(row_b, I * items) - i * items) & (
            lax.rem(row_b, I * items) // items == i
        )
        back = back + dot_nn(pick.astype(F32).astype(BF16), down[i])
    back_out[...] = back.reshape(back_out.shape).astype(BF16)
    for n in range(1, E):
        spread_expert(back_out, back_in, s_back, r_back, n, "start")
    pass_on(2, 1, 1, "start")
    back_in[e] = back_out[e]
    turned = pltpu.roll(gate_table, lax.rem(128 - c * (I * 2 * items), 128), 1)
    for n in range(1, E):
        spread_expert(back_out, back_in, s_back, r_back, n, "recv")
    for s in range(E):
        value = jnp.zeros((total, rows), F32)
        given = back_in[s].astype(F32)
        for i in range(I):
            for j in range(items):
                lane = i * 2 * items + j
                value = value + turned[:, lane : lane + 1] * given[i * items + j : i * items + j + 1, :]
        comb[c, s] = value.astype(BF16)
    for n in range(1, C):
        gather_cache(comb, s_comb, r_comb, n, "start")
    put_together(2)
    for n in range(1, C):
        gather_cache(comb, s_comb, r_comb, n, "recv")
    pieces = []
    for s in range(E):
        value = comb[0, s].astype(F32)
        for m in range(1, C):
            value = value + comb[m, s].astype(F32)
        pieces.append(value)
    mixed_ref[...] = attention + jnp.concatenate(pieces, axis=1)

    for w in range(3):
        for i in range(I):
            for o in range(O):
                hop(w, i, o, "send")
                pass_on(w, o, i, "send")
            for kd in range(NEAR):
                direct(w, i, kd, "send")
    for n in range(1, C):
        part(n, "send")
        gather_cache(proj, s_proj, r_proj, n, "send")
        gather_cache(slots_all, s_slot, r_slot, n, "send")
        gather_cache(comb, s_comb, r_comb, n, "send")
    for n in range(1, E):
        spread_expert(out_slots, slots_all.at[c], s_disp, r_disp, n, "send")
        spread_expert(back_out, back_in, s_back, r_back, n, "send")
    for n in range(E):
        hidden(n, "send")


def store_kernel(S, R, g_ref, u_ref, d_ref, mixed_ref, go_hbm, uo_hbm, do_hbm, mo_ref, sems):
    height = g_ref.shape[0] // 5
    copies = [
        pltpu.make_async_copy(source.at[pl.ds(m * height, height)], target.at[pl.ds(m * height, height)], sems.at[n, m])
        for n, (source, target) in enumerate(((g_ref, go_hbm), (u_ref, uo_hbm), (d_ref, do_hbm)))
        for m in range(5)
    ]
    for copy in copies:
        copy.start()
    for s in range(S):
        mo_ref[s] = mixed_ref[s * R : (s + 1) * R, :].astype(BF16)
    for copy in copies:
        copy.wait()


def whole_shards(
    queries, k_cache, v_cache, lengths, w_out, norm_gain, w_gate, w_up, w_down, expert_ids, gate_weights
):
    C = lax.axis_size("cache")
    E = lax.axis_size("expert")
    I, rows, hidden_width = w_gate.shape
    width = hidden_width // C
    S, R = queries.shape[0], queries.shape[1]
    positions = k_cache.shape[1]
    d_model = E * rows
    cap = 2
    items = S * cap
    O = C - NEAR
    chunk = 256 * (-(-d_model // (256 * C)))
    shape = jax.ShapeDtypeStruct
    any_spec = pl.BlockSpec(memory_space=pl.ANY)
    vmem = pl.BlockSpec(memory_space=pltpu.VMEM)
    smem = pl.BlockSpec(memory_space=pltpu.SMEM)
    V = pltpu.VMEM
    sem = pltpu.SemaphoreType.DMA
    per_row = QH // KVH * S
    lines = rows // 128 * width + -(-width // 128) * (rows % 128)
    gate, up, down, mixed = pl.pallas_call(
        functools.partial(whole_kernel, C, E, I, S, R, cap),
        out_shape=(
            pltpu.VMEM((width, d_model), BF16),
            pltpu.VMEM((width, d_model), BF16),
            pltpu.VMEM((width, d_model), BF16),
            pltpu.VMEM((S * R, d_model), F32),
        ),
        in_specs=[smem, smem, smem] + [any_spec] * 8,
        out_specs=(vmem,) * 4,
        scratch_shapes=[
            V((I, rows, hidden_width), BF16),
            V((I, rows, hidden_width), BF16),
            V((I, C, width, rows), BF16),
            V((I, C, lines, 128), BF16),
            V((I, C, lines, 128), BF16),
            V((I, C, lines, 128), BF16),
            V((O, I, lines, 128), BF16),
            V((O, I, lines, 128), BF16),
            V((O, I, lines, 128), BF16),
            V((E, lines, 128), BF16),
            V((E, lines, 128), BF16),
            V((E, lines, 128), BF16),
            V(k_cache.shape, BF16),
            V(v_cache.shape, BF16),
            V((d_model, w_out.shape[0]), BF16),
            V(queries.shape, BF16),
            V((d_model,), F32),
            V((S * R, QH * HD), F32),
            V((C, R * per_row, 128), F32),
            V((C, R * per_row, 128), F32),
            V((C, S * R, d_model), F32),
            V((S * R, C * chunk), F32),
            V((E, 2 * items, chunk // 2), BF16),
            V((C, E, 2 * items, chunk // 2), BF16),
            V((E * items, C * chunk), BF16),
            V((E * items, width), BF16),
            V((I, C, E * items, width), BF16),
            V((E, I * items, rows), BF16),
            V((E, I * items, rows), BF16),
            V((C, E, S * R, rows), BF16),
            sem((4, 2)),
            sem((2, R)),
            sem((3, I, O)),
            sem((3, O, I)),
            sem((O,)),
            sem((3, I, NEAR)),
            sem((3, O, I)),
            sem((3, E)),
            sem((3,)),
            sem((C,)),
            sem((C,)),
            sem((C,)),
            sem((C,)),
            sem((E,)),
            sem((E,)),
            sem((C,)),
            sem((C,)),
            sem((E,)),
            sem((I, C)),
            sem((E,)),
            sem((E,)),
            sem((C,)),
            sem((C,)),
        ],
        compiler_params=pltpu.CompilerParams(
            collective_id=0, has_side_effects=True, vmem_limit_bytes=54 << 20
        ),
    )(
        lengths,
        expert_ids,
        gate_weights,
        queries,
        norm_gain,
        k_cache,
        v_cache,
        w_out.T,
        w_gate,
        w_up,
        w_down.reshape(I, C, width, rows),
    )
    gate, up, down, mixed = (pltpu.with_memory_space_constraint(a, pltpu.VMEM) for a in (gate, up, down, mixed))
    gate, up, down, mixed = pl.pallas_call(
        functools.partial(store_kernel, S, R),
        out_shape=(
            shape((width, d_model), BF16),
            shape((width, d_model), BF16),
            shape((width, d_model), BF16),
            shape((S, R, d_model), BF16),
        ),
        in_specs=[vmem] * 4,
        out_specs=(any_spec,) * 3 + (vmem,),
        scratch_shapes=[sem((3, 5))],
        compiler_params=pltpu.CompilerParams(vmem_limit_bytes=2 << 20),
    )(gate, up, down, mixed)
    return (
        mixed,
        gate.T.reshape(1, d_model, width),
        up.T.reshape(1, d_model, width),
        down.reshape(1, width, d_model),
    )


def exchange_plain(w_gate, w_up, w_down):
    gate_owner, up_owner = (
        lax.all_to_all(
            lax.all_to_all(w, "cache", split_axis=2, concat_axis=0, tiled=True),
            "expert",
            split_axis=0,
            concat_axis=1,
            tiled=True,
        )
        for w in (w_gate, w_up)
    )
    down_owner = lax.all_to_all(
        lax.all_to_all(w_down, "cache", split_axis=1, concat_axis=0, tiled=True),
        "expert",
        split_axis=0,
        concat_axis=2,
        tiled=True,
    )
    return gate_owner, up_owner, down_owner


def plain_shards(
    queries,
    k_cache,
    v_cache,
    lengths,
    w_out,
    norm_gain,
    w_gate,
    w_up,
    w_down,
    expert_ids,
    gate_weights,
):
    gate_owner, up_owner, down_owner = exchange_plain(w_gate, w_up, w_down)
    cache_count = lax.axis_size("cache")
    cache_place = lax.axis_index("cache")
    step_count = queries.shape[0]
    row_count = k_cache.shape[0]
    positions = k_cache.shape[1]
    group_size = QH // KVH
    heads = queries.reshape(step_count, row_count, KVH, group_size, HD).transpose(1, 2, 0, 3, 4)
    same = jnp.eye(KVH, dtype=jnp.float32)
    spread = heads[:, :, :, :, None, :] * same.astype(heads.dtype)[None, :, None, None, :, None]
    spread = spread.reshape(row_count, step_count * QH, KVH * HD)
    scores = jnp.einsum(
        "rnk,rpk->rnp", spread, k_cache, preferred_element_type=jnp.float32
    ) * (1.0 / math.sqrt(HD))
    position = cache_place * positions + jnp.arange(positions, dtype=jnp.int32)
    limit = lengths[:, None] + jnp.arange(step_count, dtype=jnp.int32)[None, :] + 1
    limit = jnp.broadcast_to(
        limit[:, None, :, None], (row_count, KVH, step_count, group_size)
    ).reshape(row_count, step_count * QH)
    visible = position[None, None, :] < limit[:, :, None]
    highest = jnp.max(jnp.where(visible, scores, -1e30), axis=-1)
    weights = jnp.where(visible, jnp.exp(scores - highest[..., None]), 0.0)
    mass = jnp.sum(weights, axis=-1)
    accum = jnp.einsum(
        "rnp,rpk->rnk",
        weights.astype(jnp.bfloat16),
        v_cache,
        preferred_element_type=jnp.float32,
    ).reshape(row_count, KVH, step_count, group_size, KVH, HD)
    accum = jnp.sum(accum * same[None, :, None, None, :, None], axis=4)

    def by_step(a):
        return jnp.moveaxis(a, 2, 0).reshape(step_count, row_count, -1)

    accum = by_step(accum)
    highest = by_step(highest.reshape(row_count, KVH, step_count, group_size))
    mass = by_step(mass.reshape(row_count, KVH, step_count, group_size))
    own_width = w_out.shape[0]
    gathered = lax.all_gather(jnp.concatenate((accum, highest, mass), axis=-1), "cache")
    own_heads = own_width // HD
    all_high = gathered[..., QH * HD : QH * HD + QH]
    factor = jnp.exp(all_high - jnp.max(all_high, axis=0))
    all_mass = jnp.sum(gathered[..., QH * HD + QH :] * factor, axis=0)
    own_factor = lax.dynamic_slice_in_dim(factor / all_mass, cache_place * own_heads, own_heads, 3)
    own_accum = lax.dynamic_slice_in_dim(gathered, cache_place * own_width, own_width, 3)
    own_out = jnp.sum(own_accum * jnp.repeat(own_factor, HD, axis=-1), axis=0)
    own_rows = own_out.astype(jnp.bfloat16).reshape(step_count * row_count, own_width)
    projected = jnp.dot(own_rows, w_out, preferred_element_type=jnp.float32)
    attention = jnp.sum(lax.all_gather(projected, "cache"), axis=0)
    scale = lax.rsqrt(jnp.mean(attention * attention, axis=-1, keepdims=True) + 1e-05)
    normed = (attention * scale * norm_gain).astype(jnp.bfloat16).reshape(step_count, row_count, D)
    experts_total = w_gate.shape[0] * cache_count
    capacity = max(2, (row_count * TOP + experts_total - 1) // experts_total)
    expert_range = jnp.arange(experts_total, dtype=jnp.int32)
    onehot = (expert_ids[..., None] == expert_range).astype(jnp.float32)
    chosen = jnp.sum(onehot, axis=2)
    gate_map = jnp.sum(onehot * gate_weights[..., None], axis=2)
    earlier = jnp.tril(jnp.ones((row_count, row_count), jnp.float32), -1)
    ranks = jnp.einsum("rq,sqe->sre", earlier, chosen, precision=lax.Precision.HIGHEST)
    slot_table = (ranks[..., None] == jnp.arange(capacity, dtype=jnp.float32)).astype(
        jnp.float32
    ) * chosen[..., None]
    outgoing = jnp.einsum(
        "srec,srd->escd",
        slot_table.astype(jnp.bfloat16),
        normed,
        preferred_element_type=jnp.float32,
    )
    outgoing = outgoing.astype(jnp.bfloat16).reshape(experts_total, step_count * capacity, D)
    slots = lax.all_to_all(outgoing, "expert", split_axis=0, concat_axis=0, tiled=True)
    source_count = slots.shape[0]
    item_count = slots.shape[1]
    slot_rows = slots.reshape(source_count * item_count, D)
    gate_value = jnp.dot(slot_rows, gate_owner[0], preferred_element_type=jnp.float32)
    up_value = jnp.dot(slot_rows, up_owner[0], preferred_element_type=jnp.float32)
    hidden = (jax.nn.silu(gate_value) * up_value).astype(jnp.bfloat16)
    partial_out = jnp.dot(hidden, down_owner[0], preferred_element_type=jnp.float32).reshape(
        source_count, item_count, D
    )
    expert_out = partial_out.astype(jnp.bfloat16)
    returned = lax.all_to_all(expert_out, "expert", split_axis=0, concat_axis=0, tiled=True)
    back_width = returned.shape[-1]
    returned = returned.reshape(experts_total, step_count, capacity, back_width)
    combined = jnp.einsum(
        "srec,escd->srd",
        slot_table * gate_map[..., None],
        returned.astype(jnp.float32),
        precision=lax.Precision.HIGHEST,
    )
    attention_rows = attention.reshape(step_count, row_count, D)
    combined = jnp.sum(lax.all_gather(combined, "cache"), axis=0)
    mixed = (attention_rows + combined).astype(jnp.bfloat16)
    return (mixed, gate_owner, up_owner, down_owner)


def shards(*args):
    queries, w_out, w_gate = args[0], args[4], args[6]
    C, E = lax.axis_size("cache"), lax.axis_size("expert")
    I, rows, hidden_width = w_gate.shape
    fits = (
        C % NEAR == 0
        and C == 2 * NEAR
        and C == KVH
        and I * C == E
        and rows % 8 == 0
        and rows % 128 > 0
        and rows > 128
        and hidden_width % (40 * C) == 0
        and w_out.shape[0] * C == QH * HD
        and queries.shape[0] * queries.shape[1] == 8
        and I * queries.shape[0] * 2 == 8
        and 2 * queries.shape[0] * 2 == 8
        and queries.shape[1] * TOP <= 2 * E
    )
    return (whole_shards if fits else plain_shards)(*args)


def solution(mesh):
    return jax.shard_map(
        shards,
        mesh=mesh,
        in_specs=(
            P(None, "expert", None),
            P("expert", "cache", None),
            P("expert", "cache", None),
            P("expert"),
            P("cache", None),
            P(),
            P("cache", "expert", None),
            P("cache", "expert", None),
            P("cache", None, "expert"),
            P(None, "expert", None),
            P(None, "expert", None),
        ),
        out_specs=(
            P(None, "expert", None),
            P("expert", None, "cache"),
            P("expert", None, "cache"),
            P("expert", "cache", None),
        ),
        check_vma=False,
    )
```
